32 devices in a mesh: dp: 8 (over y, x, core), tensor: 4 (over z).
Axes of the slice: x: 2, y: 2, z: 4, core: 2. Of those that a mesh axis runs over, the one named last changes fastest.
Arguments:
- hidden_in: bfloat16 [1024, 2048], P('dp'), may hold values from -6 to 6
- attn_gain: float32 [2048], replicated, may hold values from 0.5 to 1.5
- query_weight: bfloat16 [2048, 2048], P('dp', 'tensor'), may hold values from -0.125 to 0.125
- key_weight: bfloat16 [2048, 2048], P('dp', 'tensor'), may hold values from -0.125 to 0.125
- value_weight: bfloat16 [2048, 2048], P('dp', 'tensor'), may hold values from -0.125 to 0.125
- output_weight: bfloat16 [2048, 2048], P('dp', 'tensor'), may hold values from -1.5 to 1.5
- query_gain: float32 [2048], P('tensor'), may hold values from 0.5 to 1.5
- key_gain: float32 [2048], P('tensor'), may hold values from 0.5 to 1.5
- moe_gain: float32 [2048], replicated, may hold values from 0.5 to 1.5
- expert_gate_up: bfloat16 [2048, 16, 2, 1024], P(None, 'dp', None, 'tensor'), may hold values from -0.125 to 0.125
- expert_down: bfloat16 [2048, 16, 1024], P(None, 'dp', 'tensor'), may hold values from -0.1875 to 0.1875
- experts: int32 [1024, 8], P('dp'), may hold values from 0 to 15, all different within a row
- gates: float32 [1024, 8], P('dp'), may hold values from 0.25 to 0.75
- anchor: int32 [1024], P('dp'), may hold values from 0 to 1023, each once
- lengths: int32 [4], replicated, may hold values from 1 to 512, 1024 in all
- cotangent: bfloat16 [1024, 2048], P('dp'), may hold values from -8 to 8
Outputs:
- output: bfloat16 [1024, 2048], P('dp')
- input_grad: float32 [1024, 2048], P('dp')
- query_grad: float32 [2048, 2048], P('dp', 'tensor')
- key_grad: float32 [2048, 2048], P('dp', 'tensor')
- value_grad: float32 [2048, 2048], P('dp', 'tensor')
- output_grad: float32 [2048, 2048], P('dp', 'tensor')
- gate_up_grad: float32 [2048, 16, 2, 1024], P(None, 'dp', None, 'tensor')
- down_grad: float32 [2048, 16, 1024], P(None, 'dp', 'tensor')
- attn_gain_grad: float32 [2048], P('dp')
- query_gain_grad: float32 [2048], P('dp')
- key_gain_grad: float32 [2048], P('dp')
- moe_gain_grad: float32 [2048], P('dp')
The draws below stay inside these ranges and needn't reach their ends.
Inputs may be any that keep to these rules, and one draw needn't show every extreme that they name: `anchor`: each number appears once. The lengths sum to 1024; the longest is exactly 512. Each row names 8 different experts.
All inputs are finite; a program needn't handle non-finite values.
Results may differ from the reference program's by a relative error of at most 0.033.
Values may be sent and summed in bfloat16 or wider, within the bound.
A program may use at most 256 MiB of HBM per device.

```python
import math
import jax
import jax.numpy as jnp
import numpy as np
from jax import lax

D = 2048
HEADS = 16
HD = 128
FF = 1024
TOPK = 8
TOK_DEV = 128
E = 16
TOKENS = 1024
MAXLEN = 512
NSEQ = 4
CAP = 72
N_DP = 8


def draw_cotangent(key, part):
    row_index = jnp.arange(TOKENS, dtype=jnp.float32)
    row_scale = 0.6 + 1.2 * row_index / TOKENS
    values = jax.random.normal(key, (TOKENS, D), jnp.float32) * row_scale[:, None]
    return jnp.clip(values, -8.0, 8.0).astype(jnp.bfloat16)


def steps_of(own_key, shape, pieces, least, largest):
    def one(dim, shards_of):
        draws = jax.random.uniform(jax.random.fold_in(jax.random.fold_in(own_key, 6), dim), (shards_of,), jnp.float32, least / len(pieces), largest / len(pieces))
        return jnp.repeat(jnp.exp(draws), shape[dim] // shards_of).reshape((-1,) + (1,) * (len(shape) - dim - 1))

    loudness = one(*pieces[0])
    for cut in pieces[1:]:
        loudness = loudness * one(*cut)
    return loudness


def picks_of(rng, rows, number_of, top, lift):
    ranking = jax.random.permutation(jax.random.fold_in(rng, 1), number_of)
    favour = ranking
    for power in range(3):
        favour = favour * favour // number_of
    favour = favour * lift // number_of
    tickets = jax.random.randint(jax.random.fold_in(rng, 2), (rows, number_of), 0, 4096) + favour
    sure = jax.random.permutation(jax.random.fold_in(rng, 3), rows)[jnp.arange(number_of) % rows]
    tickets = jnp.where(jnp.arange(rows)[:, None] == sure[None, :], 1 << 14, tickets)
    score = tickets * number_of + jnp.arange(number_of)
    return lax.top_k(score.astype(jnp.int32), top)[1].astype(jnp.int32)


def split_up(amount, total, most, slope):
    portions = [(1 << 20) // math.isqrt(rank ** slope) + 1 for rank in range(2, amount + 1)]
    spare, counts = total - most - (amount - 1), [1] * (amount - 1)
    while spare > 0:
        free = [i for i in range(amount - 1) if counts[i] < most]
        pool, left = sum([portions[i] for i in free]), spare
        for i in free:
            addition = min(most - counts[i], max(1, left * portions[i] // pool), spare)
            counts[i] = counts[i] + addition
            spare = spare - addition
    return np.array([most] + counts)


def ragged(rng, number_of, total, reach, skew):
    if number_of == 2:
        one = jax.random.randint(rng, (), max(1, total - reach), min(reach, total - 1) + 1)
        return jnp.stack([one, total - one])
    tallies = jnp.asarray(split_up(number_of, total, reach, skew), jnp.int32)
    couples = (number_of - 1) // 2
    giver, sink = tallies[1:1 + 2 * couples:2], tallies[2:2 + 2 * couples:2]
    slack = jnp.minimum(giver - 1, reach - sink)
    moved = jax.random.randint(jax.random.fold_in(rng, 1), (couples,), 0, 1 << 20) % (slack + 1)
    tallies = tallies.at[1:1 + 2 * couples:2].set(giver - moved).at[2:2 + 2 * couples:2].set(sink + moved)
    return tallies[jax.random.permutation(jax.random.fold_in(rng, 2), number_of)]


def gaussian(key, extent, scale, reach, shards=(), held_as=jnp.bfloat16):
    drawn = scale * jax.random.normal(key, extent, jnp.float32)
    if shards:
        drawn = drawn * steps_of(key, extent, shards, -0.22, 0.18)
    return jnp.clip(drawn, -reach, reach).astype(held_as)


def setup_inputs(seed: int = 0) -> dict:
    seeds = jax.random.split(jax.random.key(seed), 17)
    hidden_in = gaussian(seeds[0], (TOKENS, D), 1.0, 6.0, ((0, 8),))
    attn_gain = jnp.clip(1.0 + 0.1 * jax.random.normal(seeds[1], (D,), jnp.float32), 0.5, 1.5)
    query_weight = gaussian(seeds[2], (D, D), D ** -0.5, 0.125, ((0, 8), (1, 4)))
    key_weight = gaussian(seeds[3], (D, D), D ** -0.5, 0.125, ((0, 8), (1, 4)))
    value_weight = gaussian(seeds[4], (D, D), D ** -0.5, 0.125, ((0, 8), (1, 4)))
    output_weight = gaussian(seeds[5], (D, D), (max(D // 128, HD // 8)) ** -0.5, 1.5, ((0, 8), (1, 4)))
    query_gain = jnp.clip(1.0 + 0.1 * jax.random.normal(seeds[6], (D,), jnp.float32), 0.5, 1.5)
    key_gain = jnp.clip(1.0 + 0.1 * jax.random.normal(seeds[7], (D,), jnp.float32), 0.5, 1.5)
    moe_gain = jnp.clip(1.0 + 0.1 * jax.random.normal(seeds[8], (D,), jnp.float32), 0.5, 1.5)
    expert_gate_up = gaussian(seeds[9], (D, E, 2, FF), D ** -0.5, 0.125, ((1, 8), (3, 4)))
    expert_down = gaussian(seeds[10], (D, E, FF), FF ** -0.5, 0.1875, ((1, 8), (2, 4)))
    experts = picks_of(seeds[11], TOKENS, E, TOPK, 4096)
    gates = jnp.clip(0.25 + 0.5 * jax.random.uniform(seeds[12], (TOKENS, TOPK), jnp.float32) ** steps_of(seeds[12], (TOKENS, TOPK), ((0, 8),), -0.2, 0.2), 0.25, 0.75)
    anchor = jax.random.permutation(seeds[13], TOKENS).astype(jnp.int32)
    lengths = ragged(seeds[14], NSEQ, TOKENS, MAXLEN, 2).astype(jnp.int32)
    cotangent = draw_cotangent(jax.random.fold_in(seeds[16], 71), 0)
    return {"hidden_in": hidden_in, "attn_gain": attn_gain, "query_weight": query_weight, "key_weight": key_weight, "value_weight": value_weight, "output_weight": output_weight, "query_gain": query_gain, "key_gain": key_gain, "moe_gain": moe_gain, "expert_gate_up": expert_gate_up, "expert_down": expert_down, "experts": experts, "gates": gates, "anchor": anchor, "lengths": lengths, "cotangent": cotangent}


EPSILON = 1e-05
ROPE_BASE = 10000.0
HIGH_PREC = lax.Precision.HIGHEST
NEG_FILL = -1e+30

@jax.custom_vjp
def low(v):
    return lax.optimization_barrier(v.astype(jnp.bfloat16)).astype(jnp.float32)

@jax.custom_vjp
def low_back(v):
    return v

def low_keep(v):
    return (low(v), None)

def low_pass(kept, grad):
    return (grad,)

def back_keep(v):
    return (v, None)

def back_low(kept, grad):
    return (low(grad),)
low.defvjp(low_keep, low_pass)
low_back.defvjp(back_keep, back_low)

def rms_norm(values, gain):
    return values * lax.rsqrt(lax.optimization_barrier(jnp.mean(values * values, axis=-1, keepdims=True)) + EPSILON) * gain

def locate(anchor, lengths):
    ends = jnp.cumsum(lengths).astype(jnp.int32)
    starts = (ends - lengths).astype(jnp.int32)
    docs = lax.optimization_barrier(jnp.sum((anchor[:, None] >= ends[None, :]).astype(jnp.int32), axis=1)).astype(jnp.int32)
    which = docs[:, None] == jnp.arange(lengths.shape[0], dtype=jnp.int32)[None, :]
    begins = lax.optimization_barrier(jnp.sum(jnp.where(which, starts[None, :], 0), axis=1)).astype(jnp.int32)
    return (docs, (anchor - begins).astype(jnp.int32))

def rotary(tensor, positions):
    half_dim = HD // 2
    freqs = ROPE_BASE ** (-2.0 * jnp.arange(half_dim, dtype=jnp.float32) / HD)
    angles = positions.astype(jnp.float32)[:, None] * freqs[None, :]
    cosine = jnp.cos(angles)[:, None, :]
    sine_part = jnp.sin(angles)[:, None, :]
    first_half = tensor[..., :half_dim]
    second_half = tensor[..., half_dim:]
    return jnp.concatenate([first_half * cosine - second_half * sine_part, second_half * cosine + first_half * sine_part], axis=-1)

def routing(expert_rows, gate_rows):
    tok_count = expert_rows.shape[0]
    flat_ids = expert_rows.reshape(-1)
    one_hot = (flat_ids[:, None] == jnp.arange(E, dtype=jnp.int32)[None, :]).astype(jnp.int32)
    earlier = (jnp.cumsum(one_hot, axis=0) - one_hot).astype(jnp.int32)
    slot_ids = lax.optimization_barrier(jnp.sum(earlier * one_hot, axis=1)).astype(jnp.int32)
    dest_rows = jnp.where(slot_ids < CAP, flat_ids * CAP + slot_ids, E * CAP).astype(jnp.int32)
    pair_token = (jnp.arange(tok_count * TOPK, dtype=jnp.int32) // TOPK).astype(jnp.int32)
    slot_source = jnp.zeros((E * CAP + 1,), jnp.int32).at[dest_rows].set(pair_token)
    slot_filled = jnp.zeros((E * CAP + 1,), jnp.float32).at[dest_rows].set(1.0)
    slot_gate = jnp.zeros((E * CAP + 1,), jnp.float32).at[dest_rows].set(gate_rows.reshape(-1))
    return (dest_rows, slot_source[:-1], slot_filled[:-1], slot_gate[:-1])

def attend(query_rows, key_rows, value_rows, docs):
    qblock = min(512, TOKENS)
    pad_key = jnp.concatenate([jnp.zeros((MAXLEN, HEADS, HD), key_rows.dtype), key_rows], axis=0)
    pad_value = jnp.concatenate([jnp.zeros((MAXLEN, HEADS, HD), value_rows.dtype), value_rows], axis=0)
    pad_docs = jnp.concatenate([jnp.full((MAXLEN,), -1, jnp.int32), docs], axis=0)
    score_scale = HD ** (-0.5)

    def one_block(offset):
        query_part = lax.dynamic_slice_in_dim(query_rows, offset, qblock, 0)
        key_part = lax.dynamic_slice_in_dim(pad_key, offset, MAXLEN + qblock, 0)
        value_part = lax.dynamic_slice_in_dim(pad_value, offset, MAXLEN + qblock, 0)
        query_docs = lax.dynamic_slice_in_dim(docs, offset, qblock, 0)
        key_docs = lax.dynamic_slice_in_dim(pad_docs, offset, MAXLEN + qblock, 0)
        query_index = offset + jnp.arange(qblock, dtype=jnp.int32)
        key_index = offset - MAXLEN + jnp.arange(MAXLEN + qblock, dtype=jnp.int32)
        allowed = ((query_docs[:, None] == key_docs[None, :]) & (key_index[None, :] <= query_index[:, None]))[None]
        scores = low_back(score_scale * jnp.einsum('qhd,khd->hqk', query_part, key_part, precision=HIGH_PREC))
        scores = jnp.where(allowed, scores, NEG_FILL)
        log_total = jax.nn.logsumexp(scores, axis=-1, keepdims=True)
        attn_probs = jnp.where(allowed, jnp.exp(scores - log_total), 0.0)
        return jnp.einsum('hqk,khd->qhd', low(attn_probs), value_part, precision=HIGH_PREC)
    offsets = jnp.arange(TOKENS // qblock, dtype=jnp.int32) * qblock
    result = lax.map(jax.checkpoint(one_block), offsets)
    return result.reshape(TOKENS, HEADS, HD)

def expert_shard(moe_rows, dest_rows, slot_source, slot_filled, gate_rows, gateup_w, down_w):
    buffer_rows = (moe_rows[slot_source] * slot_filled[:, None]).reshape(E, CAP, D)
    gate_up = low_back(jnp.einsum('ecd,dezf->eczf', buffer_rows, gateup_w, precision=HIGH_PREC))
    activated = low(jax.nn.silu(gate_up[:, :, 0]) * gate_up[:, :, 1])
    expert_out = low_back(jnp.einsum('ecf,def->ecd', activated, down_w, precision=HIGH_PREC))
    table_rows = jnp.concatenate([expert_out.reshape(E * CAP, D), jnp.zeros((1, D), expert_out.dtype)], axis=0)
    return lax.optimization_barrier(jnp.sum(table_rows[dest_rows].reshape(-1, TOPK, D) * gate_rows[:, :, None], axis=1))

def reference(hidden_in, attn_gain, query_weight, key_weight, value_weight, output_weight, query_gain, key_gain, moe_gain, expert_gate_up, expert_down, experts, gates, anchor, lengths, cotangent):
    docs_stream, unused = locate(jnp.arange(TOKENS, dtype=jnp.int32), lengths)
    docs, positions = locate(anchor, lengths)
    inverse = jnp.zeros((TOKENS,), jnp.int32).at[anchor].set(jnp.arange(TOKENS, dtype=jnp.int32))
    routes = jax.vmap(routing)(experts.reshape(N_DP, TOK_DEV, TOPK), gates.reshape(N_DP, TOK_DEV, TOPK))
    dest_rows, slot_source, slot_filled, unused_gate = routes
    gate_values = gates.astype(jnp.float32)

    def forward(inputs, norm_gain, query_w, key_w, value_w, output_w, qgain, kgain, mgain, gateup_w, down_w):
        normed = low(rms_norm(inputs, norm_gain))
        query_raw = low_back(jnp.dot(normed, query_w, precision=HIGH_PREC))
        key_raw = low_back(jnp.dot(normed, key_w, precision=HIGH_PREC))
        value_raw = low(low_back(jnp.dot(normed, value_w, precision=HIGH_PREC)))
        query_hat = rms_norm(query_raw, qgain)
        key_hat = rms_norm(key_raw, kgain)
        query_rows = low(rotary(query_hat.reshape(TOKENS, HEADS, HD), positions))
        key_rows = low(rotary(key_hat.reshape(TOKENS, HEADS, HD), positions))
        value_rows = value_raw.reshape(TOKENS, HEADS, HD)
        mixed = attend(query_rows[inverse], key_rows[inverse], value_rows[inverse], docs_stream)[anchor]
        mixed = low(low_back(mixed.reshape(TOKENS, D)))
        residual = inputs + low_back(jnp.dot(mixed, output_w.T, precision=HIGH_PREC))
        moe_in = low(rms_norm(residual, mgain))

        def per_shard(packed):
            return jax.checkpoint(expert_shard)(packed[0], packed[1], packed[2], packed[3], packed[4], gateup_w, down_w)
        combined = lax.map(per_shard, (moe_in.reshape(N_DP, TOK_DEV, D), dest_rows, slot_source, slot_filled, gate_values.reshape(N_DP, TOK_DEV, TOPK)))
        return residual + combined.reshape(TOKENS, D)
    floats = tuple((item.astype(jnp.float32) for item in (hidden_in, attn_gain, query_weight, key_weight, value_weight, output_weight, query_gain, key_gain, moe_gain, expert_gate_up, expert_down)))
    result, pullback = jax.vjp(forward, *floats)
    grads = pullback(cotangent.astype(jnp.float32))
    return (result.astype(jnp.bfloat16), grads[0], grads[2], grads[3], grads[4], grads[5], grads[9], grads[10], grads[1], grads[6], grads[7], grads[8])
```

```python
import functools
import jax
import jax.numpy as jnp
from jax import lax
from jax.experimental import pallas as pl
from jax.experimental.pallas import tpu as pltpu
from jax.sharding import PartitionSpec as P

MESH = pl.DeviceIdType.MESH
f32 = jnp.float32
bf16 = jnp.bfloat16


def bit_list(n):
    bits, b = [], 1
    while b < n:
        bits.append(b)
        b *= 2
    return bits


def flip(i, m):
    for b in bit_list(m + 1):
        if m & b:
            i = i + b - 2 * b * ((i // b) % 2)
    return i


def span(bits):
    out = [0]
    for b in bits:
        out = out + [m | b for m in out]
    return out


def orders(n):
    bits = bit_list(n)
    outer = bits[1:]
    return (outer + bits[:1], outer[::-1] + bits[:1])


def hello(peers):
    barrier = pltpu.get_barrier_semaphore()
    for peer in peers:
        pl.semaphore_signal(barrier, inc=1, device_id=peer, device_id_type=MESH)
    pl.semaphore_wait(barrier, len(peers))


def rdma(src, dst, send_sem, recv_sem, peer):
    return pltpu.make_async_remote_copy(
        src_ref=src, dst_ref=dst, send_sem=send_sem, recv_sem=recv_sem,
        device_id=peer, device_id_type=MESH,
    )


class Gather:
    def __init__(self, n, me, src, dst, send_sems, recv_sems):
        self.n, self.me, self.src, self.dst = n, me, src, dst
        self.send_sems, self.recv_sems = send_sems, recv_sems
        self.half = src.shape[0] // 2
        self.sent = []

    def push(self, h, m, bit):
        rows = pl.ds(h * self.half, self.half)
        place = self.dst(flip(self.me, m)).at[rows]
        copy = rdma(self.src.at[rows] if m == 0 else place, place, self.send_sems.at[h, m | bit],
                    self.recv_sems.at[h, m | bit], {"dp": flip(self.me, bit)})
        copy.start()
        self.sent.append(copy)

    def start(self):
        o = orders(self.n)
        for j in range(len(o[0])):
            for h in (0, 1):
                self.push(h, 0, o[h][j])

    def stage(self, j):
        o = orders(self.n)
        for i in range(2**j):
            for h in (0, 1):
                m = span(o[h][:j])[i] | o[h][j]
                place = self.dst(flip(self.me, m)).at[pl.ds(h * self.half, self.half)]
                rdma(place, place, self.send_sems.at[h, m], self.recv_sems.at[h, m],
                     {"dp": flip(self.me, o[h][j])}).wait_recv()
                for bit in o[h][j + 1:]:
                    self.push(h, m, bit)

    def finish(self):
        for copy in self.sent:
            copy.wait_send()


def dp_peers(n, me):
    return [{"dp": flip(me, b)} for b in bit_list(n)]


def all_peers(axis, n, me):
    return [{axis: flip(me, m)} for m in range(1, n)]


def call(kernel, name, cid, outs, out_space, in_space, scratch, *args):
    single = not isinstance(outs, (list, tuple))
    spec = pl.BlockSpec(memory_space=out_space)
    return pl.pallas_call(
        kernel,
        out_shape=outs,
        in_specs=[pl.BlockSpec(memory_space=in_space)] * len(args),
        out_specs=spec if single else [spec] * len(outs),
        scratch_shapes=scratch,
        compiler_params=pltpu.CompilerParams(collective_id=cid, has_side_effects=True),
        name=name,
    )(*args)


def gather_kernel(n, count, *refs):
    srcs, dsts, sems = refs[:count], refs[count:2 * count], refs[2 * count:]
    me = lax.axis_index("dp")
    own = [pltpu.make_async_copy(srcs[i], dsts[i].at[me], sems[2 * count].at[i]) for i in range(count)]
    hello(dp_peers(n, me))
    gathers = [Gather(n, me, srcs[i], (lambda o, i=i: dsts[i].at[o]), sems[2 * i], sems[2 * i + 1]) for i in range(count)]
    for g in gathers:
        g.start()
    for c in own:
        c.start()
    for j in range(len(bit_list(n))):
        for g in gathers:
            g.stage(j)
    for g in gathers:
        g.finish()
    for c in own:
        c.wait()


def gather_dp(n, arrs, cid):
    arrs = list(arrs)
    scratch = [pltpu.SemaphoreType.DMA((2, n))] * (2 * len(arrs)) + [pltpu.SemaphoreType.DMA((len(arrs),))]
    outs = [jax.ShapeDtypeStruct((n,) + a.shape, a.dtype) for a in arrs]
    return call(functools.partial(gather_kernel, n, len(arrs)), "gather_dp", cid, outs, pl.ANY, pl.ANY, scratch, *arrs)


def spread_kernel(n, nt, src, dst, zs, zr, gs, gr, loc):
    d, t = lax.axis_index("dp"), lax.axis_index("tensor")
    own = pltpu.make_async_copy(src, dst.at[d, t], loc)
    hello(dp_peers(n, d) + all_peers("tensor", nt, t))
    sent = []
    for m in range(1, nt):
        c = rdma(src, dst.at[d, t], zs.at[m], zr.at[m], {"tensor": flip(t, m)})
        c.start()
        sent.append(c)
    gathers = []
    for m in range(nt):
        tm = flip(t, m)
        gathers.append(Gather(n, d, src if m == 0 else dst.at[d, tm], (lambda o, tm=tm: dst.at[o, tm]), gs.at[m], gr.at[m]))
    gathers[0].start()
    own.start()
    for m in range(1, nt):
        place = dst.at[d, flip(t, m)]
        rdma(place, place, zs.at[m], zr.at[m], {"tensor": flip(t, m)}).wait_recv()
        gathers[m].start()
        gathers[m - 1].stage(0)
        if m > 1:
            gathers[m - 2].stage(1)
    steps = len(bit_list(n))
    done = [0] * nt
    for m in range(nt):
        done[m] = 0 if m == nt - 1 else 1 if m == nt - 2 else 2
    for j in range(steps):
        for m in range(nt):
            if done[m] == j:
                gathers[m].stage(j)
                done[m] = j + 1
    for g in gathers:
        g.finish()
    for c in sent:
        c.wait_send()
    own.wait()


def spread(n, nt, x, cid):
    scratch = [pltpu.SemaphoreType.DMA((nt,))] * 2 + [pltpu.SemaphoreType.DMA((nt, 2, n))] * 2 + [pltpu.SemaphoreType.DMA]
    out = jax.ShapeDtypeStruct((n, nt) + x.shape, x.dtype)
    return call(functools.partial(spread_kernel, n, nt), "spread", cid, out, pl.ANY, pl.ANY, scratch, x)


def reduce_dp(n, me, p_ref, acc, got, send_sems, recv_sems, put):
    half = p_ref.shape[1] // 2
    bits = bit_list(n)
    o = [x[::-1] for x in orders(n)]
    sent = []
    base = 0
    for j in range(len(bits)):
        keeps = [span(o[h][j + 1:]) for h in (0, 1)]
        for i in range(len(keeps[0])):
            for h in (0, 1):
                m, b = keeps[h][i], o[h][j]
                src = p_ref.at[flip(me, m | b), pl.ds(h * half, half)] if j == 0 else acc.at[h, m | b]
                c = rdma(src, got.at[h, base + i], send_sems.at[h, base + i], recv_sems.at[h, base + i], {"dp": flip(me, b)})
                c.start()
                sent.append(c)
        for i in range(len(keeps[0]))[::-1]:
            for h in (0, 1):
                m, b = keeps[h][i], o[h][j]
                rows = pl.ds(h * half, half)
                view = got.at[h, base + i]
                rdma(view, view, send_sems.at[h, base + i], recv_sems.at[h, base + i], {"dp": flip(me, b)}).wait_recv()
                mine = p_ref[flip(me, m), rows] if j == 0 else acc[h, m]
                total = mine.astype(f32) + view[...].astype(f32)
                if j == len(bits) - 1:
                    put(rows, total)
                else:
                    acc[h, m] = total.astype(bf16)
        base += len(keeps[0])
    return sent


def fold_kernel(n, nt, p_ref, out_ref, acc, got, part, zgot, send_sems, recv_sems, zs, zr):
    d, t = lax.axis_index("dp"), lax.axis_index("tensor")
    hello(dp_peers(n, d) + all_peers("tensor", nt, t))
    share = out_ref.shape[0]

    def put(rows, total):
        part[rows, :] = total.astype(bf16)

    sent = reduce_dp(n, d, p_ref, acc, got, send_sems, recv_sems, put)
    for m in range(1, nt):
        c = rdma(part.at[pl.ds(flip(t, m) * share, share)], zgot.at[m], zs.at[m], zr.at[m], {"tensor": flip(t, m)})
        c.start()
        sent.append(c)
    total = part[pl.ds(t * share, share), :].astype(f32)
    for m in range(1, nt):
        rdma(zgot.at[m], zgot.at[m], zs.at[m], zr.at[m], {"tensor": flip(t, m)}).wait_recv()
        total = total + zgot[m].astype(f32)
    out_ref[...] = total
    for c in sent:
        c.wait_send()


def fold(n, nt, p, cid):
    _, rows, cols = p.shape
    scratch = [
        pltpu.VMEM((2, n, rows // 2, cols), bf16),
        pltpu.VMEM((2, n, rows // 2, cols), bf16),
        pltpu.VMEM((rows, cols), bf16),
        pltpu.VMEM((nt, rows // nt, cols), bf16),
    ] + [pltpu.SemaphoreType.DMA((2, n))] * 2 + [pltpu.SemaphoreType.DMA((nt,))] * 2
    out = jax.ShapeDtypeStruct((rows // nt, cols), f32)
    return call(functools.partial(fold_kernel, n, nt), "fold", cid, out, pltpu.VMEM, pltpu.VMEM, scratch, p)


def zsum_kernel(nt, x_ref, out_ref, zgot, zs, zr):
    t = lax.axis_index("tensor")
    hello(all_peers("tensor", nt, t))
    share = out_ref.shape[0]
    sent = []
    for m in range(1, nt):
        c = rdma(x_ref.at[pl.ds(flip(t, m) * share, share)], zgot.at[m], zs.at[m], zr.at[m], {"tensor": flip(t, m)})
        c.start()
        sent.append(c)
    total = x_ref[pl.ds(t * share, share), :].astype(f32)
    for m in range(1, nt):
        rdma(zgot.at[m], zgot.at[m], zs.at[m], zr.at[m], {"tensor": flip(t, m)}).wait_recv()
        total = total + zgot[m].astype(f32)
    out_ref[...] = total
    for c in sent:
        c.wait_send()


def zsum(nt, x, cid):
    rows, cols = x.shape
    scratch = [pltpu.VMEM((nt, rows // nt, cols), x.dtype)] + [pltpu.SemaphoreType.DMA((nt,))] * 2
    out = jax.ShapeDtypeStruct((rows // nt, cols), f32)
    return call(functools.partial(zsum_kernel, nt), "zsum", cid, out, pltpu.VMEM, pltpu.VMEM, scratch, x)


def direct_kernel(axis, n, split, count, *refs):
    srcs, dsts, ss, rs, loc = refs[:count], refs[count:2 * count], *refs[2 * count:]
    me = lax.axis_index(axis)
    own = [pltpu.make_async_copy(srcs[i].at[me] if split else srcs[i], dsts[i].at[me], loc.at[i]) for i in range(count)]
    hello(all_peers(axis, n, me))
    sent = []
    for m in range(1, n):
        for i in range(count):
            peer = flip(me, m)
            c = rdma(srcs[i].at[peer] if split else srcs[i], dsts[i].at[me], ss.at[i, m], rs.at[i, m], {axis: peer})
            c.start()
            sent.append(c)
    for c in own:
        c.start()
    for m in range(1, n):
        for i in range(count):
            place = dsts[i].at[flip(me, m)]
            rdma(place, place, ss.at[i, m], rs.at[i, m], {axis: flip(me, m)}).wait_recv()
    for c in sent:
        c.wait_send()
    for c in own:
        c.wait()


def direct(axis, n, arrs, cid, split=False):
    arrs = list(arrs)
    scratch = [pltpu.SemaphoreType.DMA((len(arrs), n))] * 2 + [pltpu.SemaphoreType.DMA((len(arrs),))]
    outs = [jax.ShapeDtypeStruct(a.shape if split else (n,) + a.shape, a.dtype) for a in arrs]
    return call(functools.partial(direct_kernel, axis, n, split, len(arrs)), "direct_" + axis, cid, outs, pltpu.VMEM, pltpu.VMEM, scratch, *arrs)


D = 2048
HD = 128
TOPK = 8
EPSILON = 1e-05
ROPE_BASE = 10000.0
NEG_FILL = -1e30


def norm_back(values, gain, grad_out):
    inv_rms = lax.rsqrt(jnp.mean(values * values, axis=-1, keepdims=True) + EPSILON)
    weighted = grad_out * gain
    grad_in = inv_rms * weighted - values * inv_rms**3 * jnp.mean(weighted * values, axis=-1, keepdims=True)
    return grad_in, jnp.sum(grad_out * values * inv_rms, axis=0)


def locate(anchor, lengths):
    ends = jnp.cumsum(lengths)
    starts = ends - lengths
    docs = jnp.sum((anchor[:, None] >= ends[None, :]).astype(jnp.int32), axis=1)
    which = docs[:, None] == jnp.arange(lengths.shape[0], dtype=jnp.int32)[None, :]
    begins = jnp.sum(jnp.where(which, starts[None, :], 0), axis=1)
    return docs, (anchor - begins).astype(jnp.int32)


def rope_tables(positions):
    half_dim = HD // 2
    freqs = ROPE_BASE ** (-2.0 * jnp.arange(half_dim, dtype=f32) / HD)
    angles = positions.astype(f32)[:, None] * freqs[None, :]
    cosine, sine = jnp.cos(angles), jnp.sin(angles)
    return jnp.concatenate([cosine, cosine], axis=1)[:, None, :], jnp.concatenate([-sine, sine], axis=1)[:, None, :]


def turn(x, cosine, sine):
    return x * cosine + jnp.roll(x, HD // 2, axis=-1) * sine


def pair_allowed(query_anchor, query_docs, key_anchor, key_docs):
    return ((query_docs[:, None] == key_docs[None, :]) & (key_anchor[None, :] <= query_anchor[:, None]))[None]


def contract(left, right, l, r):
    return lax.dot_general(left, right, (((l,), (r,)), ((), ())), preferred_element_type=f32)


def routing(experts, gates, num_exp, capacity):
    toks = experts.shape[0]
    chosen = experts[:, :, None] == jnp.arange(num_exp, dtype=jnp.int32)[None, None, :]
    mask = jnp.any(chosen, axis=1)
    gate = jnp.sum(jnp.where(chosen, gates[:, :, None], 0.0), axis=1)
    index = jnp.arange(toks, dtype=jnp.int32)
    before = (index[:, None] > index[None, :]).astype(bf16)
    slot = contract(before, mask.astype(bf16), 1, 0)
    return jnp.where(mask & (slot < capacity), gate, 0.0)


def small(rows):
    rows = jnp.stack(rows)
    return jnp.pad(rows, ((0, -rows.shape[0] % 8), (0, 0)))


def shards(hidden_in, attn_gain, query_weight, key_weight, value_weight, output_weight, query_gain, key_gain,
           moe_gain, expert_gate_up, expert_down, experts, gates, anchor, lengths, cotangent):
    n, nt = lax.axis_size("dp"), lax.axis_size("tensor")
    d, t = lax.axis_index("dp"), lax.axis_index("tensor")
    toks = hidden_in.shape[0]
    share = toks // nt
    cols = query_weight.shape[1]
    heads = cols // HD
    scale = HD ** (-0.5)
    exp_local = expert_down.shape[1]
    num_exp = exp_local * n
    capacity = 9 * toks * TOPK // (8 * num_exp)
    hidden = hidden_in.astype(f32)

    def mine(a):
        return lax.dynamic_slice_in_dim(a, t * share, share, 0)

    coef = routing(experts, gates, num_exp, capacity).T
    place = jnp.broadcast_to(anchor[None, :], (16, toks))
    wq, wk, wv, wo, dy_all, coef_all, anchor_all = gather_dp(
        n, (query_weight, key_weight, value_weight, output_weight, cotangent, coef, place), 1)
    wq, wk, wv, wo = (w.reshape(D, cols) for w in (wq, wk, wv, wo))
    dy_all = dy_all.reshape(n * toks, D)
    coef_all = lax.dynamic_slice_in_dim(coef_all, d * exp_local, exp_local, 1)
    coef_all = coef_all.transpose(0, 2, 1).reshape(n * toks, exp_local)
    anchor_all = anchor_all[:, 0].reshape(n * toks)

    docs, positions = locate(anchor, lengths)
    docs_all, _ = locate(anchor_all, lengths)
    cosine, sine = rope_tables(positions)
    allowed = pair_allowed(anchor, docs, anchor_all, docs_all)
    allowed_back = pair_allowed(anchor_all, docs_all, anchor, docs)

    inv = lax.rsqrt(jnp.mean(hidden * hidden, axis=-1, keepdims=True) + EPSILON)
    normed = (hidden * inv * attn_gain).astype(bf16)
    q_raw, k_raw, v_raw = (contract(normed, w, 1, 0) for w in (wq, wk, wv))
    (sq,) = direct("tensor", nt, [small([jnp.sum(q_raw * q_raw, axis=1), jnp.sum(k_raw * k_raw, axis=1)])], 2)
    sq = jnp.sum(sq, axis=0)
    q_inv = lax.rsqrt(sq[0] / D + EPSILON)[:, None]
    k_inv = lax.rsqrt(sq[1] / D + EPSILON)[:, None]
    q = turn((q_raw * q_inv * query_gain).reshape(toks, heads, HD), cosine, sine).astype(bf16)
    k = turn((k_raw * k_inv * key_gain).reshape(toks, heads, HD), cosine, sine).astype(bf16)
    v = v_raw.astype(bf16)
    k_all, v_all = gather_dp(n, (k.reshape(toks, cols), v), 3)
    k_all, v_all = (a.reshape(n * toks, heads, HD) for a in (k_all, v_all))
    v = v.reshape(toks, heads, HD)

    scores = scale * jnp.einsum("qhd,khd->hqk", q, k_all, preferred_element_type=f32)
    top = jnp.max(jnp.where(allowed, scores, NEG_FILL), axis=2)
    probs = jnp.where(allowed, jnp.exp(scores - top[:, :, None]), 0.0)
    total = jnp.sum(probs, axis=2)
    lse = top + jnp.log(total)
    attended = jnp.einsum("hqk,khd->qhd", probs.astype(bf16), v_all, preferred_element_type=f32)
    attended = attended / total.T[:, :, None]
    o = attended.reshape(toks, cols).astype(bf16)
    h1 = mine(hidden) + zsum(nt, contract(o, wo, 1, 1).astype(bf16), 4)
    n2 = (h1 * lax.rsqrt(jnp.mean(h1 * h1, axis=-1, keepdims=True) + EPSILON) * moe_gain).astype(bf16)
    n2_all = spread(n, nt, n2, 5).reshape(n * toks, D)

    gu = jnp.einsum("td,dezf->tezf", n2_all, expert_gate_up, preferred_element_type=f32)
    g, u = gu[:, :, 0], gu[:, :, 1]
    sig = jax.nn.sigmoid(g)
    act = (coef_all[:, :, None] * (g * sig * u)).astype(bf16)
    dact = coef_all[:, :, None] * jnp.einsum("td,def->tef", dy_all, expert_down, preferred_element_type=f32)
    dgu = jnp.stack([dact * u * sig * (1.0 + g * (1.0 - sig)), dact * (g * sig)], axis=2).astype(bf16)
    dn2 = jnp.einsum("tezf,dezf->td", dgu, expert_gate_up, preferred_element_type=f32).astype(bf16)
    moe = jnp.einsum("tef,def->td", act, expert_down, preferred_element_type=f32).astype(bf16)
    down_grad = jnp.einsum("td,tef->def", dy_all, act, preferred_element_type=f32)
    gate_up_grad = jnp.einsum("td,tezf->dezf", n2_all, dgu, preferred_element_type=f32)

    dn2 = fold(n, nt, dn2.reshape(n, toks, D), 6)
    dres, moe_gain_part = norm_back(h1, moe_gain, dn2)
    dh1 = mine(cotangent).astype(f32) + dres
    moe = fold(n, nt, moe.reshape(n, toks, D), 7)
    out_share = (h1 + moe).astype(bf16)
    dh1r, output = direct("tensor", nt, [dh1.astype(bf16), out_share], 8)
    dh1r = dh1r.reshape(toks, D)
    output = output.reshape(toks, D)

    do = contract(dh1r, wo, 1, 0).astype(bf16)
    delta = jnp.sum(do.reshape(toks, heads, HD).astype(f32) * attended, axis=2).T
    stats = small(list(lse) + list(delta))
    if stats.shape[0] % 16:
        stats = jnp.pad(stats, ((0, 8), (0, 0)))
    q_all, do_all, o_all, stats_all = gather_dp(n, (q.reshape(toks, cols), do, o, stats), 9)
    slices, = direct("dp", n, [jnp.concatenate([normed, dh1r], axis=0).reshape(2 * toks, n, D // n).transpose(1, 0, 2)], 10, True)
    normed_all = slices[:, :toks].reshape(n * toks, D // n)
    dh1r_all = slices[:, toks:].reshape(n * toks, D // n)
    output_grad = contract(dh1r_all, o_all.reshape(n * toks, cols), 0, 0)

    do = do.reshape(toks, heads, HD)
    q_all, do_all = (a.reshape(n * toks, heads, HD) for a in (q_all, do_all))
    lse_all = stats_all[:, :heads].transpose(1, 0, 2).reshape(heads, n * toks)
    delta_all = stats_all[:, heads:2 * heads].transpose(1, 0, 2).reshape(heads, n * toks)
    probs = jnp.where(allowed, jnp.exp(scores - lse[:, :, None]), 0.0)
    dprobs = jnp.einsum("qhd,khd->hqk", do, v_all, preferred_element_type=f32)
    ds = (probs * (dprobs - delta[:, :, None])).astype(bf16)
    dq = scale * jnp.einsum("hqk,khd->qhd", ds, k_all, preferred_element_type=f32)
    scores_b = scale * jnp.einsum("qhd,khd->hqk", q_all, k, preferred_element_type=f32)
    probs_b = jnp.where(allowed_back, jnp.exp(scores_b - lse_all[:, :, None]), 0.0)
    dv = jnp.einsum("hqk,qhd->khd", probs_b.astype(bf16), do_all, preferred_element_type=f32)
    dprobs_b = jnp.einsum("qhd,khd->hqk", do_all, v, preferred_element_type=f32)
    ds_b = (probs_b * (dprobs_b - delta_all[:, :, None])).astype(bf16)
    dk = scale * jnp.einsum("hqk,qhd->khd", ds_b, q_all, preferred_element_type=f32)
    dq_hat = turn(dq, cosine, -sine).reshape(toks, cols)
    dk_hat = turn(dk, cosine, -sine).reshape(toks, cols)
    dv = dv.reshape(toks, cols).astype(bf16)

    wdq, wdk = dq_hat * query_gain, dk_hat * key_gain
    q_gain_part = jnp.sum(dq_hat * q_raw * q_inv, axis=0)
    k_gain_part = jnp.sum(dk_hat * k_raw * k_inv, axis=0)
    (cross,) = direct("tensor", nt, [small([jnp.sum(wdq * q_raw, axis=1), jnp.sum(wdk * k_raw, axis=1)])], 11)
    cross = jnp.sum(cross, axis=0)
    dq_raw = (q_inv * wdq - q_raw * q_inv**3 * cross[0][:, None] / D).astype(bf16)
    dk_raw = (k_inv * wdk - k_raw * k_inv**3 * cross[1][:, None] / D).astype(bf16)
    dnormed = contract(dq_raw, wq, 1, 1) + contract(dk_raw, wk, 1, 1) + contract(dv, wv, 1, 1)
    dnormed = zsum(nt, dnormed.astype(bf16), 12)
    dx, attn_gain_part = norm_back(mine(hidden), attn_gain, dnormed)

    def wide(part):
        return lax.dynamic_update_slice_in_dim(jnp.zeros((D,), f32), part, t * cols, 0)

    gains = small([attn_gain_part, wide(q_gain_part), wide(k_gain_part), moe_gain_part])
    gains = jnp.concatenate([gains, jnp.zeros_like(gains)], axis=0)
    dq_all, dk_all, dv_all, gains_all = gather_dp(n, (dq_raw, dk_raw, dv, gains), 13)
    query_grad, key_grad, value_grad = (
        contract(normed_all, a.reshape(n * toks, cols), 0, 0) for a in (dq_all, dk_all, dv_all))
    gains = lax.dynamic_slice_in_dim(jnp.sum(gains_all[:, :8], axis=0), d * (D // n), D // n, 1)
    input_grad, gains = direct("tensor", nt, [(dh1 + dx).astype(bf16), gains], 14)
    input_grad = input_grad.reshape(toks, D).astype(f32)
    gains = jnp.sum(gains, axis=0)
    return (output, input_grad, query_grad, key_grad, value_grad, output_grad, gate_up_grad, down_grad,
            gains[0], gains[1], gains[2], gains[3])


def solution(mesh):
    in_specs = (
        P("dp", None),
        P(),
        P("dp", "tensor"),
        P("dp", "tensor"),
        P("dp", "tensor"),
        P("dp", "tensor"),
        P("tensor"),
        P("tensor"),
        P(),
        P(None, "dp", None, "tensor"),
        P(None, "dp", "tensor"),
        P("dp", None),
        P("dp", None),
        P("dp"),
        P(),
        P("dp", None),
    )
    out_specs = (
        P("dp", None),
        P("dp", None),
        P("dp", "tensor"),
        P("dp", "tensor"),
        P("dp", "tensor"),
        P("dp", "tensor"),
        P(None, "dp", None, "tensor"),
        P(None, "dp", "tensor"),
        P("dp"),
        P("dp"),
        P("dp"),
        P("dp"),
    )
    return jax.shard_map(shards, mesh=mesh, in_specs=in_specs, out_specs=out_specs, check_vma=False)
```

```python
import functools
import jax
import jax.numpy as jnp
from jax import lax
from jax.experimental import pallas as pl
from jax.experimental.pallas import tpu as pltpu
from jax.sharding import PartitionSpec as P

MESH = pl.DeviceIdType.MESH
f32 = jnp.float32
bf16 = jnp.bfloat16


def bit_list(n):
    bits, b = [], 1
    while b < n:
        bits.append(b)
        b *= 2
    return bits


def flip(i, m):
    for b in bit_list(m + 1):
        if m & b:
            i = i + b - 2 * b * ((i // b) % 2)
    return i


def span(bits):
    out = [0]
    for b in bits:
        out = out + [m | b for m in out]
    return out


def orders(n):
    bits = bit_list(n)
    outer = bits[1:]
    return (outer + bits[:1], outer[::-1] + bits[:1])


def hello(peers):
    barrier = pltpu.get_barrier_semaphore()
    for peer in peers:
        pl.semaphore_signal(barrier, inc=1, device_id=peer, device_id_type=MESH)
    pl.semaphore_wait(barrier, len(peers))


def rdma(src, dst, send_sem, recv_sem, peer):
    return pltpu.make_async_remote_copy(
        src_ref=src, dst_ref=dst, send_sem=send_sem, recv_sem=recv_sem,
        device_id=peer, device_id_type=MESH,
    )


class Gather:
    def __init__(self, n, me, src, dst, send_sems, recv_sems):
        self.n, self.me, self.src, self.dst = n, me, src, dst
        self.send_sems, self.recv_sems = send_sems, recv_sems
        self.half = src.shape[0] // 2
        self.sent = []

    def push(self, h, m, bit):
        rows = pl.ds(h * self.half, self.half)
        place = self.dst(flip(self.me, m)).at[rows]
        copy = rdma(self.src.at[rows] if m == 0 else place, place, self.send_sems.at[h, m | bit],
                    self.recv_sems.at[h, m | bit], {"dp": flip(self.me, bit)})
        copy.start()
        self.sent.append(copy)

    def start(self):
        o = orders(self.n)
        for j in range(len(o[0])):
            for h in (0, 1):
                self.push(h, 0, o[h][j])

    def stage(self, j):
        o = orders(self.n)
        for i in range(2**j):
            for h in (0, 1):
                m = span(o[h][:j])[i] | o[h][j]
                place = self.dst(flip(self.me, m)).at[pl.ds(h * self.half, self.half)]
                rdma(place, place, self.send_sems.at[h, m], self.recv_sems.at[h, m],
                     {"dp": flip(self.me, o[h][j])}).wait_recv()
                for bit in o[h][j + 1:]:
                    self.push(h, m, bit)

    def finish(self):
        for copy in self.sent:
            copy.wait_send()


def dp_peers(n, me):
    return [{"dp": flip(me, b)} for b in bit_list(n)]


def all_peers(axis, n, me):
    return [{axis: flip(me, m)} for m in range(1, n)]


def call(kernel, name, cid, outs, out_space, in_space, scratch, *args):
    single = not isinstance(outs, (list, tuple))
    spec = pl.BlockSpec(memory_space=out_space)
    return pl.pallas_call(
        kernel,
        out_shape=outs,
        in_specs=[pl.BlockSpec(memory_space=in_space)] * len(args),
        out_specs=spec if single else [spec] * len(outs),
        scratch_shapes=scratch,
        compiler_params=pltpu.CompilerParams(collective_id=cid, has_side_effects=True),
        name=name,
    )(*args)


def gather_kernel(n, count, *refs):
    srcs, dsts, sems = refs[:count], refs[count:2 * count], refs[2 * count:]
    me = lax.axis_index("dp")
    own = [pltpu.make_async_copy(srcs[i], dsts[i].at[me], sems[2 * count].at[i]) for i in range(count)]
    hello(dp_peers(n, me))
    gathers = [Gather(n, me, srcs[i], (lambda o, i=i: dsts[i].at[o]), sems[2 * i], sems[2 * i + 1]) for i in range(count)]
    for g in gathers:
        g.start()
    for c in own:
        c.start()
    for j in range(len(bit_list(n))):
        for g in gathers:
            g.stage(j)
    for g in gathers:
        g.finish()
    for c in own:
        c.wait()


def gather_dp(n, arrs, cid):
    arrs = list(arrs)
    scratch = [pltpu.SemaphoreType.DMA((2, n))] * (2 * len(arrs)) + [pltpu.SemaphoreType.DMA((len(arrs),))]
    outs = [jax.ShapeDtypeStruct((n,) + a.shape, a.dtype) for a in arrs]
    return call(functools.partial(gather_kernel, n, len(arrs)), "gather_dp", cid, outs, pl.ANY, pl.ANY, scratch, *arrs)


class Spread:
    def __init__(self, n, nt, d, t, src, dst, zs, zr, gs, gr):
        self.nt, self.t, self.d, self.src, self.dst, self.zs, self.zr = nt, t, d, src, dst, zs, zr
        self.steps = len(bit_list(n))
        self.gathers = []
        for m in range(nt):
            tm = flip(t, m)
            own = src if m == 0 else dst.at[d, tm]
            self.gathers.append(Gather(n, d, own, (lambda o, tm=tm: dst.at[o, tm]), gs.at[m], gr.at[m]))
        self.sent = []

    def start(self):
        for m in range(1, self.nt):
            c = rdma(self.src, self.dst.at[self.d, self.t], self.zs.at[m], self.zr.at[m], {"tensor": flip(self.t, m)})
            c.start()
            self.sent.append(c)
        self.gathers[0].start()

    def run(self):
        done = [0] * self.nt
        for m in range(1, self.nt):
            place = self.dst.at[self.d, flip(self.t, m)]
            rdma(place, place, self.zs.at[m], self.zr.at[m], {"tensor": flip(self.t, m)}).wait_recv()
            self.gathers[m].start()
            for k in range(m):
                if done[k] < self.steps and k + done[k] < m:
                    self.gathers[k].stage(done[k])
                    done[k] += 1
        for j in range(self.steps):
            for m in range(self.nt):
                if done[m] == j:
                    self.gathers[m].stage(j)
                    done[m] = j + 1

    def finish(self):
        for g in self.gathers:
            g.finish()
        for c in self.sent:
            c.wait_send()


class Reduce:
    def __init__(self, n, me, p, got, send_sems, recv_sems):
        self.n, self.me, self.p, self.got, self.ss, self.rs = n, me, p, got, send_sems, recv_sems
        self.half = p.shape[1] // 2
        self.bits = len(bit_list(n))
        self.o = [x[::-1] for x in orders(n)]
        self.keeps = [[span(self.o[h][j + 1:]) for h in (0, 1)] for j in range(self.bits)]
        self.base = [sum(len(self.keeps[k][0]) for k in range(j)) for j in range(self.bits)]
        self.sent = []

    def piece(self, j, h, m):
        if j == 0:
            return self.p.at[flip(self.me, m), pl.ds(h * self.half, self.half)]
        return self.got.at[h, self.base[j - 1] + self.keeps[j - 1][h].index(m)]

    def each(self, j):
        for i in range(len(self.keeps[j][0])):
            for h in (0, 1):
                yield h, self.keeps[j][h][i], self.o[h][j], self.base[j] + i

    def send(self, j):
        for h, m, b, k in self.each(j):
            c = rdma(self.piece(j, h, m | b), self.got.at[h, k], self.ss.at[h, k], self.rs.at[h, k], {"dp": flip(self.me, b)})
            c.start()
            self.sent.append(c)

    def recv(self, j, put=None):
        for h, m, b, k in self.each(j):
            view = self.got.at[h, k]
            rdma(view, view, self.ss.at[h, k], self.rs.at[h, k], {"dp": flip(self.me, b)}).wait_recv()
            total = self.piece(j, h, m)[...].astype(f32) + view[...].astype(f32)
            if j == self.bits - 1:
                put(pl.ds(h * self.half, self.half), total)
            else:
                view[...] = total.astype(bf16)

    def finish(self):
        for c in self.sent:
            c.wait_send()


class ZSum:
    def __init__(self, nt, t, src, got, zs, zr):
        self.nt, self.t, self.src, self.got, self.zs, self.zr = nt, t, src, got, zs, zr
        self.share = src.shape[0] // nt
        self.sent = []

    def start(self):
        for m in range(1, self.nt):
            peer = flip(self.t, m)
            c = rdma(self.src.at[pl.ds(peer * self.share, self.share)], self.got.at[m], self.zs.at[m], self.zr.at[m], {"tensor": peer})
            c.start()
            self.sent.append(c)

    def total(self):
        total = self.src[pl.ds(self.t * self.share, self.share), :].astype(f32)
        for m in range(1, self.nt):
            v = self.got.at[m]
            rdma(v, v, self.zs.at[m], self.zr.at[m], {"tensor": flip(self.t, m)}).wait_recv()
            total = total + v[...].astype(f32)
        return total

    def finish(self):
        for c in self.sent:
            c.wait_send()


class Direct:
    def __init__(self, axis, n, me, src, dst, ss, rs, split=False):
        self.axis, self.n, self.me, self.src, self.dst, self.ss, self.rs, self.split = axis, n, me, src, dst, ss, rs, split
        self.sent = []

    def start(self):
        for m in range(1, self.n):
            peer = flip(self.me, m)
            c = rdma(self.src.at[peer] if self.split else self.src, self.dst.at[self.me], self.ss.at[m], self.rs.at[m], {self.axis: peer})
            c.start()
            self.sent.append(c)

    def wait(self):
        for m in range(1, self.n):
            place = self.dst.at[flip(self.me, m)]
            rdma(place, place, self.ss.at[m], self.rs.at[m], {self.axis: flip(self.me, m)}).wait_recv()

    def finish(self):
        for c in self.sent:
            c.wait_send()


def greet(n, nt, d, t, every_dp=False):
    hello((all_peers("dp", n, d) if every_dp else dp_peers(n, d)) + all_peers("tensor", nt, t))


def inv_rms(v):
    return lax.rsqrt(jnp.mean(v * v, axis=-1, keepdims=True) + EPSILON)


VM = pl.BlockSpec(memory_space=pltpu.VMEM)
HB = pl.BlockSpec(memory_space=pl.ANY)
DMA = pltpu.SemaphoreType.DMA


def kernel_call(kernel, name, cid, in_specs, outs, out_specs, scratch, args):
    return pl.pallas_call(
        kernel, out_shape=outs, in_specs=in_specs, out_specs=out_specs, scratch_shapes=scratch,
        compiler_params=pltpu.CompilerParams(collective_id=cid, has_side_effects=True), name=name,
    )(*args)


def stats_kernel(n, nt, sq, wo, sq_all, wo_all, ss, rs, gs, gr, loc):
    d, t = lax.axis_index("dp"), lax.axis_index("tensor")
    greet(n, nt, d, t)
    x = Direct("tensor", nt, t, sq, sq_all, ss, rs)
    g = Gather(n, d, wo, lambda o: wo_all.at[o], gs, gr)
    own = pltpu.make_async_copy(wo, wo_all.at[d], loc)
    x.start()
    g.start()
    own.start()
    sq_all[t] = sq[...]
    x.wait()
    for j in range(len(bit_list(n))):
        g.stage(j)
    g.finish()
    x.finish()
    own.wait()


def stats(n, nt, sq, wo, cid):
    return kernel_call(
        functools.partial(stats_kernel, n, nt), "stats", cid, [VM, HB],
        [jax.ShapeDtypeStruct((nt,) + sq.shape, sq.dtype), jax.ShapeDtypeStruct((n,) + wo.shape, wo.dtype)], [VM, HB],
        [DMA((nt,)), DMA((nt,)), DMA((2, n)), DMA((2, n)), DMA], (sq, wo))


def enter_kernel(n, nt, part, hidden, gain, dy, coef, n2_all, h1, dy_all, coef_all,
                 zgot, n2, zs, zr, ps, pr, gs, gr, ys, yr, cs, cr, loc):
    d, t = lax.axis_index("dp"), lax.axis_index("tensor")
    greet(n, nt, d, t)
    z = ZSum(nt, t, part, zgot, zs, zr)
    z.start()
    gy = Gather(n, d, dy, lambda o: dy_all.at[o], ys, yr)
    gc = Gather(n, d, coef, lambda o: coef_all.at[o], cs, cr)
    gc.start()
    gy.start()
    own_y = pltpu.make_async_copy(dy, dy_all.at[d], loc.at[0])
    own_c = pltpu.make_async_copy(coef, coef_all.at[d], loc.at[1])
    own_y.start()
    own_c.start()
    value = hidden[pl.ds(t * z.share, z.share), :].astype(f32) + z.total()
    h1[...] = value
    n2[...] = (value * inv_rms(value) * gain[...]).astype(bf16)
    s = Spread(n, nt, d, t, n2, n2_all, ps, pr, gs, gr)
    own_n = pltpu.make_async_copy(n2, n2_all.at[d, t], loc.at[2])
    s.start()
    own_n.start()
    for j in range(len(bit_list(n))):
        gc.stage(j)
        gy.stage(j)
    s.run()
    s.finish()
    gy.finish()
    gc.finish()
    z.finish()
    own_y.wait()
    own_c.wait()
    own_n.wait()


def enter(n, nt, part, hidden, gain, dy, coef, cid):
    rows, cols = part.shape
    share = rows // nt
    sds = jax.ShapeDtypeStruct
    return kernel_call(
        functools.partial(enter_kernel, n, nt), "enter", cid, [VM, VM, VM, HB, HB],
        [sds((n, nt, share, cols), bf16), sds((share, cols), f32), sds((n,) + dy.shape, dy.dtype), sds((n,) + coef.shape, coef.dtype)],
        [HB, VM, HB, HB],
        [pltpu.VMEM((nt, share, cols), bf16), pltpu.VMEM((share, cols), bf16), DMA((nt,)), DMA((nt,)), DMA((nt,)), DMA((nt,)),
         DMA((nt, 2, n)), DMA((nt, 2, n)), DMA((2, n)), DMA((2, n)), DMA((2, n)), DMA((2, n)), DMA((3,))],
        (part, hidden, gain, dy, coef))


def leave_kernel(n, nt, both, *refs):
    if both:
        (dn2, moe, h1, cot, gain, dh1, dh1r_all, gain_part, moe_part,
         got, got2, part, zgot, low, ss, rs, ss2, rs2, zs, zr, xs, xr) = refs
    else:
        dn2, h1, cot, gain, dh1, dh1r_all, gain_part, got, part, zgot, low, ss, rs, zs, zr, xs, xr = refs
    d, t = lax.axis_index("dp"), lax.axis_index("tensor")
    greet(n, nt, d, t)
    steps = len(bit_list(n))

    def put(rows, total):
        part[rows, :] = total.astype(bf16)

    a = Reduce(n, d, dn2, got, ss, rs)
    z = ZSum(nt, t, part, zgot, zs, zr)
    if both:
        b = Reduce(n, d, moe, got2, ss2, rs2)

        def put2(rows, total):
            moe_part[rows, :] = total.astype(bf16)

    a.send(0)
    a.recv(0, put)
    for j in range(1, steps):
        a.send(j)
        if both and j == 1:
            b.send(0)
        a.recv(j, put)
    z.start()
    if both:
        b.recv(0, put2)
        b.send(1)
    value = h1[...]
    dz = z.total()
    r = inv_rms(value)
    weighted = dz * gain[...]
    grad = r * weighted - value * (r * r * r) * jnp.mean(weighted * value, axis=-1, keepdims=True)
    grad = cot[pl.ds(t * z.share, z.share), :].astype(f32) + grad
    dh1[...] = grad
    low[...] = grad.astype(bf16)
    dh1r_all[t] = grad.astype(bf16)
    gain_part[...] = jnp.broadcast_to(jnp.sum(dz * value * r, axis=0, keepdims=True), gain_part.shape)
    x = Direct("tensor", nt, t, low, dh1r_all, xs, xr)
    x.start()
    if both:
        for j in range(1, steps):
            b.recv(j, put2)
            if j + 1 < steps:
                b.send(j + 1)
        b.finish()
    x.wait()
    a.finish()
    z.finish()
    x.finish()


def leave(n, nt, dn2, moe, h1, cot, gain, cid):
    _, rows, cols = dn2.shape
    share = rows // nt
    sds, vm = jax.ShapeDtypeStruct, pltpu.VMEM
    both = moe is not None
    outs = [sds((share, cols), f32), sds((nt, share, cols), bf16), sds((8, cols), f32)]
    if both:
        outs.append(sds((rows, cols), bf16))
    got = [vm((2, n, rows // 2, cols), bf16)] * (2 if both else 1)
    sems = [DMA((2, n))] * (4 if both else 2) + [DMA((nt,))] * 4
    args = (dn2, moe, h1, cot, gain) if both else (dn2, h1, cot, gain)
    return kernel_call(
        functools.partial(leave_kernel, n, nt, both), "leave", cid, [VM] * len(args), outs, [VM] * len(outs),
        got + [vm((rows, cols), bf16), vm((nt, share, cols), bf16), vm((share, cols), bf16)] + sems, args)


def fold_kernel(n, nt, p, out, got, ss, rs):
    d = lax.axis_index("dp")
    hello(dp_peers(n, d))

    def put(rows, total):
        out[rows, :] = total.astype(bf16)

    a = Reduce(n, d, p, got, ss, rs)
    for j in range(len(bit_list(n))):
        a.send(j)
        a.recv(j, put)
    a.finish()


def fold(n, nt, p, cid):
    _, rows, cols = p.shape
    return kernel_call(functools.partial(fold_kernel, n, nt), "fold", cid, [VM], jax.ShapeDtypeStruct((rows, cols), bf16), VM,
                       [pltpu.VMEM((2, n, rows // 2, cols), bf16), DMA((2, n)), DMA((2, n))], (p,))


def back_kernel(n, nt, count, *refs):
    moe, h1, srcs = refs[0], refs[1], refs[2:2 + count]
    out_all, dsts = refs[2 + count], refs[3 + count:3 + 2 * count]
    zgot, low, zs, zr, xs, xr, gs, gr, loc = refs[3 + 2 * count:]
    d, t = lax.axis_index("dp"), lax.axis_index("tensor")
    greet(n, nt, d, t)
    z = ZSum(nt, t, moe, zgot, zs, zr)
    gathers = [Gather(n, d, srcs[i], (lambda o, i=i: dsts[i].at[o]), gs.at[i], gr.at[i]) for i in range(count)]
    own = [pltpu.make_async_copy(srcs[i], dsts[i].at[d], loc.at[i]) for i in range(count)]
    for g in gathers:
        g.start()
    z.start()
    for c in own:
        c.start()
    for g in gathers:
        g.stage(0)
    value = (h1[...] + z.total()).astype(bf16)
    low[...] = value
    out_all[t] = value
    x = Direct("tensor", nt, t, low, out_all, xs, xr)
    x.start()
    for j in range(1, len(bit_list(n))):
        for g in gathers:
            g.stage(j)
    x.wait()
    for g in gathers:
        g.finish()
    for c in own:
        c.wait()
    z.finish()
    x.finish()


def back(n, nt, moe, h1, arrs, cid):
    rows, cols = moe.shape
    share = rows // nt
    sds = jax.ShapeDtypeStruct
    k = len(arrs)
    return kernel_call(
        functools.partial(back_kernel, n, nt, k), "back", cid, [VM, VM] + [HB] * k,
        [sds((nt, share, cols), bf16)] + [sds((n,) + a.shape, a.dtype) for a in arrs], [VM] + [HB] * k,
        [pltpu.VMEM((nt, share, cols), bf16), pltpu.VMEM((share, cols), bf16)] + [DMA((nt,))] * 4 + [DMA((k, 2, n))] * 2 + [DMA((k,))],
        (moe, h1, *arrs))


def last_kernel(n, nt, count, *refs):
    dnormed, hidden, gain, dh1, gains, slices, srcs = *refs[:6], refs[6:6 + count]
    grad_all, gains_out, slices_all, dsts = *refs[6 + count:9 + count], refs[9 + count:9 + 2 * count]
    (zgot, low, gpart, ggot, gsum, gall, zs, zr, xs, xr, gs, gr, bs, br, ps, pr, qs, qr, loc) = refs[9 + 2 * count:]
    d, t = lax.axis_index("dp"), lax.axis_index("tensor")
    greet(n, nt, d, t, True)
    z = ZSum(nt, t, dnormed, zgot, zs, zr)
    z.start()
    gathers = [Gather(n, d, srcs[i], (lambda o, i=i: dsts[i].at[o]), gs.at[i], gr.at[i]) for i in range(count)]
    own = [pltpu.make_async_copy(srcs[i], dsts[i].at[d], loc.at[i]) for i in range(count)]
    own.append(pltpu.make_async_copy(slices.at[d], slices_all.at[d], loc.at[count]))
    for g in gathers:
        g.start()
    b = Direct("dp", n, d, slices, slices_all, bs, br, True)
    b.start()
    for c in own:
        c.start()
    for g in gathers:
        g.stage(0)
    dz = z.total()
    value = hidden[pl.ds(t * z.share, z.share), :].astype(f32)
    r = inv_rms(value)
    weighted = dz * gain[...]
    grad = r * weighted - value * (r * r * r) * jnp.mean(weighted * value, axis=-1, keepdims=True)
    grad = (dh1[...] + grad).astype(bf16)
    low[...] = grad
    grad_all[t] = grad
    x = Direct("tensor", nt, t, low, grad_all, xs, xr)
    x.start()
    row = jnp.sum(dz * value * r, axis=0, keepdims=True)
    first = lax.broadcasted_iota(jnp.int32, gains.shape, 0) == 0
    whole = jnp.where(first, row, gains[...])
    width = gpart.shape[2]
    for i in range(n):
        gpart[i] = whole[:, i * width:(i + 1) * width]
    p = Direct("dp", n, d, gpart, ggot, ps, pr, True)
    p.start()
    for j in range(1, len(bit_list(n))):
        for g in gathers:
            g.stage(j)
    p.wait()
    total = gpart[d]
    for m in range(1, n):
        total = total + ggot[flip(d, m)]
    gsum[...] = total
    gall[t] = total
    q = Direct("tensor", nt, t, gsum, gall, qs, qr)
    q.start()
    b.wait()
    x.wait()
    q.wait()
    total = gall[0]
    for i in range(1, nt):
        total = total + gall[i]
    gains_out[...] = total
    for g in gathers:
        g.finish()
    for c in own:
        c.wait()
    for e in (z, x, b, p, q):
        e.finish()


def last(n, nt, dnormed, hidden, gain, dh1, gains, slices, arrs, cid):
    rows, cols = dnormed.shape
    share = rows // nt
    width = cols // n
    sds, vm = jax.ShapeDtypeStruct, pltpu.VMEM
    k = len(arrs)
    return kernel_call(
        functools.partial(last_kernel, n, nt, k), "last", cid, [VM] * 5 + [HB] * (k + 1),
        [sds((nt, share, cols), bf16), sds((8, width), f32), sds(slices.shape, bf16)] + [sds((n,) + a.shape, a.dtype) for a in arrs],
        [VM, VM, HB] + [HB] * k,
        [vm((nt, share, cols), bf16), vm((share, cols), bf16), vm((n, 8, width), f32), vm((n, 8, width), f32), vm((8, width), f32),
         vm((nt, 8, width), f32)] + [DMA((nt,))] * 4 + [DMA((k, 2, n))] * 2 + [DMA((n,))] * 4 + [DMA((nt,))] * 2 + [DMA((k + 1,))],
        (dnormed, hidden, gain, dh1, gains, slices, *arrs))


def weight_grad_kernel(order, a_ref, b_ref, out_ref):
    res = contract(a_ref[...], b_ref[...], 0, 0)
    rows = res.shape[0]
    for c, j in enumerate(order):
        out_ref[pl.ds(j, rows, stride=len(order)), :] = res[:, c * 128:(c + 1) * 128]


def weight_grad(a, b, order):
    toks, rows = a.shape
    block = 256
    return pl.pallas_call(
        functools.partial(weight_grad_kernel, order),
        grid=(rows // block,),
        in_specs=[pl.BlockSpec((toks, block), lambda i: (0, i)), pl.BlockSpec((toks, b.shape[1]), lambda i: (0, 0))],
        out_specs=pl.BlockSpec((block * len(order), 128), lambda i: (i, 0)),
        out_shape=jax.ShapeDtypeStruct((rows * len(order), 128), f32),
        name="weight_grad",
    )(a, b)


def direct_kernel(axis, n, split, count, *refs):
    srcs, dsts, ss, rs, loc = refs[:count], refs[count:2 * count], *refs[2 * count:]
    me = lax.axis_index(axis)
    own = [pltpu.make_async_copy(srcs[i].at[me] if split else srcs[i], dsts[i].at[me], loc.at[i]) for i in range(count)]
    hello(all_peers(axis, n, me))
    sent = []
    for m in range(1, n):
        for i in range(count):
            peer = flip(me, m)
            c = rdma(srcs[i].at[peer] if split else srcs[i], dsts[i].at[me], ss.at[i, m], rs.at[i, m], {axis: peer})
            c.start()
            sent.append(c)
    for c in own:
        c.start()
    for m in range(1, n):
        for i in range(count):
            place = dsts[i].at[flip(me, m)]
            rdma(place, place, ss.at[i, m], rs.at[i, m], {axis: flip(me, m)}).wait_recv()
    for c in sent:
        c.wait_send()
    for c in own:
        c.wait()


def direct(axis, n, arrs, cid, split=False):
    arrs = list(arrs)
    scratch = [pltpu.SemaphoreType.DMA((len(arrs), n))] * 2 + [pltpu.SemaphoreType.DMA((len(arrs),))]
    outs = [jax.ShapeDtypeStruct(a.shape if split else (n,) + a.shape, a.dtype) for a in arrs]
    return call(functools.partial(direct_kernel, axis, n, split, len(arrs)), "direct_" + axis, cid, outs, pltpu.VMEM, pltpu.VMEM, scratch, *arrs)


D = 2048
HD = 128
TOPK = 8
EPSILON = 1e-05
ROPE_BASE = 10000.0
NEG_FILL = -1e30


def norm_back(values, gain, grad_out):
    inv_rms = lax.rsqrt(jnp.mean(values * values, axis=-1, keepdims=True) + EPSILON)
    weighted = grad_out * gain
    grad_in = inv_rms * weighted - values * inv_rms**3 * jnp.mean(weighted * values, axis=-1, keepdims=True)
    return grad_in, jnp.sum(grad_out * values * inv_rms, axis=0)


def locate(anchor, lengths):
    ends = jnp.cumsum(lengths)
    starts = ends - lengths
    docs = jnp.sum((anchor[:, None] >= ends[None, :]).astype(jnp.int32), axis=1)
    which = docs[:, None] == jnp.arange(lengths.shape[0], dtype=jnp.int32)[None, :]
    begins = jnp.sum(jnp.where(which, starts[None, :], 0), axis=1)
    return docs, (anchor - begins).astype(jnp.int32)


def rope_tables(positions):
    half_dim = HD // 2
    freqs = ROPE_BASE ** (-2.0 * jnp.arange(half_dim, dtype=f32) / HD)
    angles = positions.astype(f32)[:, None] * freqs[None, :]
    cosine, sine = jnp.cos(angles), jnp.sin(angles)
    return jnp.concatenate([cosine, cosine], axis=1)[:, None, :], jnp.concatenate([-sine, sine], axis=1)[:, None, :]


def turn(x, cosine, sine):
    return x * cosine + jnp.roll(x, HD // 2, axis=-1) * sine


def pair_allowed(query_anchor, query_docs, key_anchor, key_docs):
    return ((query_docs[:, None] == key_docs[None, :]) & (key_anchor[None, :] <= query_anchor[:, None]))[None]


def contract(left, right, l, r):
    return lax.dot_general(left, right, (((l,), (r,)), ((), ())), preferred_element_type=f32)


def routing(experts, gates, num_exp, capacity):
    toks = experts.shape[0]
    chosen = experts[:, :, None] == jnp.arange(num_exp, dtype=jnp.int32)[None, None, :]
    mask = jnp.any(chosen, axis=1)
    gate = jnp.sum(jnp.where(chosen, gates[:, :, None], 0.0), axis=1)
    index = jnp.arange(toks, dtype=jnp.int32)
    before = (index[:, None] > index[None, :]).astype(bf16)
    slot = contract(before, mask.astype(bf16), 1, 0)
    return jnp.where(mask & (slot < capacity), gate, 0.0)


def small(rows):
    rows = jnp.stack(rows)
    return jnp.pad(rows, ((0, -rows.shape[0] % 8), (0, 0)))


def shards(hidden_in, attn_gain, query_weight, key_weight, value_weight, output_weight, query_gain, key_gain,
           moe_gain, expert_gate_up, expert_down, experts, gates, anchor, lengths, cotangent):
    n, nt = lax.axis_size("dp"), lax.axis_size("tensor")
    d, t = lax.axis_index("dp"), lax.axis_index("tensor")
    toks = hidden_in.shape[0]
    share = toks // nt
    cols = query_weight.shape[1]
    heads = cols // HD
    scale = HD ** (-0.5)
    exp_local = expert_down.shape[1]
    num_exp = exp_local * n
    capacity = 9 * toks * TOPK // (8 * num_exp)
    hidden = hidden_in.astype(f32)

    def mine(a):
        return lax.dynamic_slice_in_dim(a, t * share, share, 0)

    coef = routing(experts, gates, num_exp, capacity).T
    place = jnp.broadcast_to(anchor[None, :], (16, toks))
    wq, wk, wv, anchor_all = gather_dp(n, (query_weight, key_weight, value_weight, place), 1)
    wq, wk, wv = (w.reshape(D, cols) for w in (wq, wk, wv))
    anchor_all = anchor_all[:, 0].reshape(n * toks)

    docs, positions = locate(anchor, lengths)
    docs_all, _ = locate(anchor_all, lengths)
    cosine, sine = rope_tables(positions)
    allowed = pair_allowed(anchor, docs, anchor_all, docs_all)
    allowed_back = pair_allowed(anchor_all, docs_all, anchor, docs)

    inv = lax.rsqrt(jnp.mean(hidden * hidden, axis=-1, keepdims=True) + EPSILON)
    normed = (hidden * inv * attn_gain).astype(bf16)
    q_raw, k_raw, v_raw = (contract(normed, w, 1, 0) for w in (wq, wk, wv))
    sq = small([jnp.sum(q_raw * q_raw, axis=1), jnp.sum(k_raw * k_raw, axis=1)])
    sq, wo = stats(n, nt, sq, output_weight, 2)
    wo = wo.reshape(D, cols)
    sq = jnp.sum(sq, axis=0)
    q_inv = lax.rsqrt(sq[0] / D + EPSILON)[:, None]
    k_inv = lax.rsqrt(sq[1] / D + EPSILON)[:, None]
    q = turn((q_raw * q_inv * query_gain).reshape(toks, heads, HD), cosine, sine).astype(bf16)
    k = turn((k_raw * k_inv * key_gain).reshape(toks, heads, HD), cosine, sine).astype(bf16)
    v = v_raw.astype(bf16)
    k_all, v_all = gather_dp(n, (k.reshape(toks, cols), v), 3)
    k_all, v_all = (a.reshape(n * toks, heads, HD) for a in (k_all, v_all))
    v = v.reshape(toks, heads, HD)

    scores = scale * jnp.einsum("qhd,khd->hqk", q, k_all, preferred_element_type=f32)
    top = jnp.max(jnp.where(allowed, scores, NEG_FILL), axis=2)
    probs = jnp.where(allowed, jnp.exp(scores - top[:, :, None]), 0.0)
    total = jnp.sum(probs, axis=2)
    lse = top + jnp.log(total)
    attended = jnp.einsum("hqk,khd->qhd", probs.astype(bf16), v_all, preferred_element_type=f32)
    attended = attended / total.T[:, :, None]
    o = attended.reshape(toks, cols).astype(bf16)
    n2_all, h1, dy_all, coef_all = enter(
        n, nt, contract(o, wo, 1, 1).astype(bf16), hidden_in, moe_gain[None, :], cotangent, coef, 4)
    n2_all, dy_all = n2_all.reshape(n * toks, D), dy_all.reshape(n * toks, D)
    coef_all = lax.dynamic_slice_in_dim(coef_all, d * exp_local, exp_local, 1)
    coef_all = coef_all.transpose(0, 2, 1).reshape(n * toks, exp_local)

    gu = jnp.einsum("td,dezf->tezf", n2_all, expert_gate_up, preferred_element_type=f32)
    g, u = gu[:, :, 0], gu[:, :, 1]
    sig = jax.nn.sigmoid(g)
    act = (coef_all[:, :, None] * (g * sig * u)).astype(bf16)
    dact = coef_all[:, :, None] * jnp.einsum("td,def->tef", dy_all, expert_down, preferred_element_type=f32)
    dgu = jnp.stack([dact * u * sig * (1.0 + g * (1.0 - sig)), dact * (g * sig)], axis=2).astype(bf16)
    dn2 = jnp.einsum("tezf,dezf->td", dgu, expert_gate_up, preferred_element_type=f32).astype(bf16)
    moe = jnp.einsum("tef,def->td", act, expert_down, preferred_element_type=f32).astype(bf16)
    half = expert_down.shape[2] // 128
    down_grad = weight_grad(dy_all, act.reshape(n * toks, -1), [f * exp_local + e for e in range(exp_local) for f in range(half)])
    down_grad = down_grad.reshape(D, half, exp_local, 128).transpose(0, 2, 1, 3).reshape(expert_down.shape)
    gate_up_grad = weight_grad(n2_all, dgu.reshape(n * toks, -1),
                               [(e * half + f) * 2 + z for e in range(exp_local) for z in (0, 1) for f in range(half)])
    gate_up_grad = gate_up_grad.reshape(D, exp_local, half, 2, 128).transpose(0, 1, 3, 2, 4).reshape(expert_gate_up.shape)

    dn2, moe = dn2.reshape(n, toks, D), moe.reshape(n, toks, D)
    together = 16 * n * toks * D <= 48 * 2**20
    dh1, dh1r, moe_gain_part, *rest = leave(n, nt, dn2, moe if together else None, h1, cotangent, moe_gain[None, :], 6)
    moe = rest[0] if together else fold(n, nt, moe, 7)
    dh1r = dh1r.reshape(toks, D)

    do = contract(dh1r, wo, 1, 0).astype(bf16)
    delta = jnp.sum(do.reshape(toks, heads, HD).astype(f32) * attended, axis=2).T
    terms = small(list(lse) + list(delta))
    if terms.shape[0] % 16:
        terms = jnp.pad(terms, ((0, 8), (0, 0)))
    output, q_all, do_all, o_all, stats_all = back(n, nt, moe, h1, (q.reshape(toks, cols), do, o, terms), 9)
    output = output.reshape(toks, D)

    do = do.reshape(toks, heads, HD)
    q_all, do_all = (a.reshape(n * toks, heads, HD) for a in (q_all, do_all))
    lse_all = stats_all[:, :heads].transpose(1, 0, 2).reshape(heads, n * toks)
    delta_all = stats_all[:, heads:2 * heads].transpose(1, 0, 2).reshape(heads, n * toks)
    probs = jnp.where(allowed, jnp.exp(scores - lse[:, :, None]), 0.0)
    dprobs = jnp.einsum("qhd,khd->hqk", do, v_all, preferred_element_type=f32)
    ds = (probs * (dprobs - delta[:, :, None])).astype(bf16)
    dq = scale * jnp.einsum("hqk,khd->qhd", ds, k_all, preferred_element_type=f32)
    scores_b = scale * jnp.einsum("qhd,khd->hqk", q_all, k, preferred_element_type=f32)
    probs_b = jnp.where(allowed_back, jnp.exp(scores_b - lse_all[:, :, None]), 0.0)
    dv = jnp.einsum("hqk,qhd->khd", probs_b.astype(bf16), do_all, preferred_element_type=f32)
    dprobs_b = jnp.einsum("qhd,khd->hqk", do_all, v, preferred_element_type=f32)
    ds_b = (probs_b * (dprobs_b - delta_all[:, :, None])).astype(bf16)
    dk = scale * jnp.einsum("hqk,qhd->khd", ds_b, q_all, preferred_element_type=f32)
    dq_hat = turn(dq, cosine, -sine).reshape(toks, cols)
    dk_hat = turn(dk, cosine, -sine).reshape(toks, cols)
    dv = dv.reshape(toks, cols).astype(bf16)

    wdq, wdk = dq_hat * query_gain, dk_hat * key_gain
    q_gain_part = jnp.sum(dq_hat * q_raw * q_inv, axis=0)
    k_gain_part = jnp.sum(dk_hat * k_raw * k_inv, axis=0)
    (cross,) = direct("tensor", nt, [small([jnp.sum(wdq * q_raw, axis=1), jnp.sum(wdk * k_raw, axis=1)])], 11)
    cross = jnp.sum(cross, axis=0)
    dq_raw = (q_inv * wdq - q_raw * q_inv**3 * cross[0][:, None] / D).astype(bf16)
    dk_raw = (k_inv * wdk - k_raw * k_inv**3 * cross[1][:, None] / D).astype(bf16)
    dnormed = contract(dq_raw, wq, 1, 1) + contract(dk_raw, wk, 1, 1) + contract(dv, wv, 1, 1)

    def wide(part):
        return lax.dynamic_update_slice_in_dim(jnp.zeros((D,), f32), part, t * cols, 0)

    gains = small([jnp.zeros((D,), f32), wide(q_gain_part), wide(k_gain_part), moe_gain_part[0]])
    slices = jnp.concatenate([normed, dh1r], axis=0).reshape(2 * toks, n, D // n).transpose(1, 0, 2)
    input_grad, gains, slices, dq_all, dk_all, dv_all = last(
        n, nt, dnormed.astype(bf16), hidden_in, attn_gain[None, :], dh1, gains, slices, (dq_raw, dk_raw, dv), 12)
    normed_all = slices[:, :toks].reshape(n * toks, D // n)
    dh1r_all = slices[:, toks:].reshape(n * toks, D // n)
    output_grad = contract(dh1r_all, o_all.reshape(n * toks, cols), 0, 0)
    query_grad, key_grad, value_grad = (
        contract(normed_all, a.reshape(n * toks, cols), 0, 0) for a in (dq_all, dk_all, dv_all))
    input_grad = input_grad.reshape(toks, D).astype(f32)
    return (output, input_grad, query_grad, key_grad, value_grad, output_grad, gate_up_grad, down_grad,
            gains[0], gains[1], gains[2], gains[3])


def solution(mesh):
    in_specs = (
        P("dp", None),
        P(),
        P("dp", "tensor"),
        P("dp", "tensor"),
        P("dp", "tensor"),
        P("dp", "tensor"),
        P("tensor"),
        P("tensor"),
        P(),
        P(None, "dp", None, "tensor"),
        P(None, "dp", "tensor"),
        P("dp", None),
        P("dp", None),
        P("dp"),
        P(),
        P("dp", None),
    )
    out_specs = (
        P("dp", None),
        P("dp", None),
        P("dp", "tensor"),
        P("dp", "tensor"),
        P("dp", "tensor"),
        P("dp", "tensor"),
        P(None, "dp", None, "tensor"),
        P(None, "dp", "tensor"),
        P("dp"),
        P("dp"),
        P("dp"),
        P("dp"),
    )
    return jax.shard_map(shards, mesh=mesh, in_specs=in_specs, out_specs=out_specs, check_vma=False)
```

```python
import functools
import jax
import jax.numpy as jnp
from jax import lax
from jax.experimental import pallas as pl
from jax.experimental.pallas import tpu as pltpu
from jax.sharding import PartitionSpec as P

MESH = pl.DeviceIdType.MESH
f32 = jnp.float32
bf16 = jnp.bfloat16


def bit_list(n):
    bits, b = [], 1
    while b < n:
        bits.append(b)
        b *= 2
    return bits


def flip(i, m):
    for b in bit_list(m + 1):
        if m & b:
            i = i + b - 2 * b * ((i // b) % 2)
    return i


def span(bits):
    out = [0]
    for b in bits:
        out = out + [m | b for m in out]
    return out


def orders(n):
    bits = bit_list(n)
    outer = bits[1:]
    return (outer + bits[:1], outer[::-1] + bits[:1])


def hello(peers):
    barrier = pltpu.get_barrier_semaphore()
    for peer in peers:
        pl.semaphore_signal(barrier, inc=1, device_id=peer, device_id_type=MESH)
    pl.semaphore_wait(barrier, len(peers))


def rdma(src, dst, send_sem, recv_sem, peer):
    return pltpu.make_async_remote_copy(
        src_ref=src, dst_ref=dst, send_sem=send_sem, recv_sem=recv_sem,
        device_id=peer, device_id_type=MESH,
    )


class Gather:
    def __init__(self, n, me, src, dst, send_sems, recv_sems):
        self.n, self.me, self.src, self.dst = n, me, src, dst
        self.send_sems, self.recv_sems = send_sems, recv_sems
        self.half = src.shape[0] // 2
        self.sent = []

    def push(self, h, m, bit):
        rows = pl.ds(h * self.half, self.half)
        place = self.dst(flip(self.me, m)).at[rows]
        copy = rdma(self.src.at[rows] if m == 0 else place, place, self.send_sems.at[h, m | bit],
                    self.recv_sems.at[h, m | bit], {"dp": flip(self.me, bit)})
        copy.start()
        self.sent.append(copy)

    def start(self):
        o = orders(self.n)
        for j in range(len(o[0])):
            for h in (0, 1):
                self.push(h, 0, o[h][j])

    def stage(self, j):
        o = orders(self.n)
        for i in range(2**j):
            for h in (0, 1):
                m = span(o[h][:j])[i] | o[h][j]
                place = self.dst(flip(self.me, m)).at[pl.ds(h * self.half, self.half)]
                rdma(place, place, self.send_sems.at[h, m], self.recv_sems.at[h, m],
                     {"dp": flip(self.me, o[h][j])}).wait_recv()
                for bit in o[h][j + 1:]:
                    self.push(h, m, bit)

    def finish(self):
        for copy in self.sent:
            copy.wait_send()


def dp_peers(n, me):
    return [{"dp": flip(me, b)} for b in bit_list(n)]


def all_peers(axis, n, me):
    return [{axis: flip(me, m)} for m in range(1, n)]


def call(kernel, name, cid, outs, out_space, in_space, scratch, *args):
    single = not isinstance(outs, (list, tuple))
    spec = pl.BlockSpec(memory_space=out_space)
    return pl.pallas_call(
        kernel,
        out_shape=outs,
        in_specs=[pl.BlockSpec(memory_space=in_space)] * len(args),
        out_specs=spec if single else [spec] * len(outs),
        scratch_shapes=scratch,
        compiler_params=pltpu.CompilerParams(collective_id=cid, has_side_effects=True),
        name=name,
    )(*args)


def gather_kernel(n, count, *refs):
    srcs, dsts, sems = refs[:count], refs[count:2 * count], refs[2 * count:]
    me = lax.axis_index("dp")
    own = [pltpu.make_async_copy(srcs[i], dsts[i].at[me], sems[2 * count].at[i]) for i in range(count)]
    hello(dp_peers(n, me))
    gathers = [Gather(n, me, srcs[i], (lambda o, i=i: dsts[i].at[o]), sems[2 * i], sems[2 * i + 1]) for i in range(count)]
    for g in gathers:
        g.start()
    for c in own:
        c.start()
    for j in range(len(bit_list(n))):
        for g in gathers:
            g.stage(j)
    for g in gathers:
        g.finish()
    for c in own:
        c.wait()


def gather_dp(n, arrs, cid):
    arrs = list(arrs)
    scratch = [pltpu.SemaphoreType.DMA((2, n))] * (2 * len(arrs)) + [pltpu.SemaphoreType.DMA((len(arrs),))]
    outs = [jax.ShapeDtypeStruct((n,) + a.shape, a.dtype) for a in arrs]
    return call(functools.partial(gather_kernel, n, len(arrs)), "gather_dp", cid, outs, pl.ANY, pl.ANY, scratch, *arrs)


class Spread:
    def __init__(self, n, nt, d, t, src, dst, zs, zr, gs, gr):
        self.nt, self.t, self.d, self.src, self.dst, self.zs, self.zr = nt, t, d, src, dst, zs, zr
        self.steps = len(bit_list(n))
        self.gathers = []
        for m in range(nt):
            tm = flip(t, m)
            own = src if m == 0 else dst.at[d, tm]
            self.gathers.append(Gather(n, d, own, (lambda o, tm=tm: dst.at[o, tm]), gs.at[m], gr.at[m]))
        self.sent = []

    def start(self):
        for m in range(1, self.nt):
            c = rdma(self.src, self.dst.at[self.d, self.t], self.zs.at[m], self.zr.at[m], {"tensor": flip(self.t, m)})
            c.start()
            self.sent.append(c)
        self.gathers[0].start()

    def run(self):
        done = [0] * self.nt
        for m in range(1, self.nt):
            place = self.dst.at[self.d, flip(self.t, m)]
            rdma(place, place, self.zs.at[m], self.zr.at[m], {"tensor": flip(self.t, m)}).wait_recv()
            self.gathers[m].start()
            for k in range(m):
                if done[k] < self.steps and k + done[k] < m:
                    self.gathers[k].stage(done[k])
                    done[k] += 1
        for j in range(self.steps):
            for m in range(self.nt):
                if done[m] == j:
                    self.gathers[m].stage(j)
                    done[m] = j + 1

    def finish(self):
        for g in self.gathers:
            g.finish()
        for c in self.sent:
            c.wait_send()


class Reduce:
    def __init__(self, n, me, p, got, send_sems, recv_sems):
        self.n, self.me, self.p, self.got, self.ss, self.rs = n, me, p, got, send_sems, recv_sems
        self.half = p.shape[1] // 2
        self.bits = len(bit_list(n))
        self.o = [x[::-1] for x in orders(n)]
        self.keeps = [[span(self.o[h][j + 1:]) for h in (0, 1)] for j in range(self.bits)]
        self.base = [sum(len(self.keeps[k][0]) for k in range(j)) for j in range(self.bits)]
        self.sent = []

    def piece(self, j, h, m):
        if j == 0:
            return self.p.at[flip(self.me, m), pl.ds(h * self.half, self.half)]
        return self.got.at[h, self.base[j - 1] + self.keeps[j - 1][h].index(m)]

    def each(self, j):
        for i in range(len(self.keeps[j][0])):
            for h in (0, 1):
                yield h, self.keeps[j][h][i], self.o[h][j], self.base[j] + i

    def send(self, j):
        for h, m, b, k in self.each(j):
            c = rdma(self.piece(j, h, m | b), self.got.at[h, k], self.ss.at[h, k], self.rs.at[h, k], {"dp": flip(self.me, b)})
            c.start()
            self.sent.append(c)

    def recv(self, j, put=None):
        for h, m, b, k in self.each(j):
            view = self.got.at[h, k]
            rdma(view, view, self.ss.at[h, k], self.rs.at[h, k], {"dp": flip(self.me, b)}).wait_recv()
            total = self.piece(j, h, m)[...].astype(f32) + view[...].astype(f32)
            if j == self.bits - 1:
                put(pl.ds(h * self.half, self.half), total)
            else:
                view[...] = total.astype(bf16)

    def finish(self):
        for c in self.sent:
            c.wait_send()


class ZSum:
    def __init__(self, nt, t, src, got, zs, zr):
        self.nt, self.t, self.src, self.got, self.zs, self.zr = nt, t, src, got, zs, zr
        self.share = src.shape[0] // nt
        self.sent = []

    def start(self):
        for m in range(1, self.nt):
            peer = flip(self.t, m)
            c = rdma(self.src.at[pl.ds(peer * self.share, self.share)], self.got.at[m], self.zs.at[m], self.zr.at[m], {"tensor": peer})
            c.start()
            self.sent.append(c)

    def total(self):
        total = self.src[pl.ds(self.t * self.share, self.share), :].astype(f32)
        for m in range(1, self.nt):
            v = self.got.at[m]
            rdma(v, v, self.zs.at[m], self.zr.at[m], {"tensor": flip(self.t, m)}).wait_recv()
            total = total + v[...].astype(f32)
        return total

    def finish(self):
        for c in self.sent:
            c.wait_send()


class Direct:
    def __init__(self, axis, n, me, src, dst, ss, rs, split=False):
        self.axis, self.n, self.me, self.src, self.dst, self.ss, self.rs, self.split = axis, n, me, src, dst, ss, rs, split
        self.sent = []

    def start(self):
        for m in range(1, self.n):
            peer = flip(self.me, m)
            c = rdma(self.src.at[peer] if self.split else self.src, self.dst.at[self.me], self.ss.at[m], self.rs.at[m], {self.axis: peer})
            c.start()
            self.sent.append(c)

    def wait(self):
        for m in range(1, self.n):
            place = self.dst.at[flip(self.me, m)]
            rdma(place, place, self.ss.at[m], self.rs.at[m], {self.axis: flip(self.me, m)}).wait_recv()

    def finish(self):
        for c in self.sent:
            c.wait_send()


def greet(n, nt, d, t, every_dp=False):
    hello((all_peers("dp", n, d) if every_dp else dp_peers(n, d)) + all_peers("tensor", nt, t))


def inv_rms(v):
    return lax.rsqrt(jnp.mean(v * v, axis=-1, keepdims=True) + EPSILON)


VM = pl.BlockSpec(memory_space=pltpu.VMEM)
HB = pl.BlockSpec(memory_space=pl.ANY)
DMA = pltpu.SemaphoreType.DMA


def kernel_call(kernel, name, cid, in_specs, outs, out_specs, scratch, args):
    return pl.pallas_call(
        kernel, out_shape=outs, in_specs=in_specs, out_specs=out_specs, scratch_shapes=scratch,
        compiler_params=pltpu.CompilerParams(collective_id=cid, has_side_effects=True), name=name,
    )(*args)


def across(column, lanes):
    return jnp.transpose(jnp.broadcast_to(column, (column.shape[0], lanes)))


def mix_kernel(n, nt, q_raw, k_raw, v, cosine, sine, q_gain, k_gain, wo, q, k, k_all, v_all, wo_all, sums,
               sq, sq_all, ss, rs, ws, wr, ks, kr, vs, vr, loc):
    d, t = lax.axis_index("dp"), lax.axis_index("tensor")
    greet(n, nt, d, t)
    row = lax.broadcasted_iota(jnp.int32, sq.shape, 0)
    part_q, part_k = (across(jnp.sum(a[...] * a[...], axis=1, keepdims=True), HD)[:8] for a in (q_raw, k_raw))
    part = jnp.where(row == 0, part_q, jnp.where(row == 1, part_k, 0.0))
    sq[...] = part
    sq_all[t] = part
    x = Direct("tensor", nt, t, sq, sq_all, ss, rs)
    x.start()
    gv = Gather(n, d, v, lambda o: v_all.at[o], vs, vr)
    gv.start()
    own = [pltpu.make_async_copy(v, v_all.at[d], loc.at[0]), pltpu.make_async_copy(wo, wo_all.at[d], loc.at[1])]
    for c in own:
        c.start()
    x.wait()
    total = sq_all[0]
    for i in range(1, nt):
        total = total + sq_all[i]
    sums[...] = total
    inv = lax.rsqrt(total / D + EPSILON)
    for i, (raw, gain, out) in enumerate(((k_raw, k_gain, k), (q_raw, q_gain, q))):
        scale = jnp.transpose(jnp.broadcast_to(inv[i ^ 1:(i ^ 1) + 1], (HD, inv.shape[1])))
        for h in range(raw.shape[1] // HD):
            at = slice(h * HD, (h + 1) * HD)
            y = raw[:, at] * scale * gain[:, at]
            out[:, at] = (y * cosine[...] + pltpu.roll(y, HD // 2, 1) * sine[...]).astype(bf16)
        if i == 0:
            gk = Gather(n, d, k, lambda o: k_all.at[o], ks, kr)
            gk.start()
            gw = Gather(n, d, wo, lambda o: wo_all.at[o], ws, wr)
            gw.start()
            own_k = pltpu.make_async_copy(k, k_all.at[d], loc.at[2])
            own_k.start()
    for j in range(len(bit_list(n))):
        for g in (gv, gk, gw):
            g.stage(j)
    for e in (x, gv, gk, gw):
        e.finish()
    for c in own:
        c.wait()
    own_k.wait()


def mix(n, nt, q_raw, k_raw, v, cosine, sine, q_gain, k_gain, wo, cid):
    toks, cols = v.shape
    sds, vm = jax.ShapeDtypeStruct, pltpu.VMEM
    wide = sds((n, toks, cols), bf16)
    return kernel_call(
        functools.partial(mix_kernel, n, nt), "mix", cid, [VM] * 7 + [HB],
        [sds((toks, cols), bf16)] * 2 + [wide, wide, sds((n,) + wo.shape, bf16), sds((8, toks), f32)], [VM] * 2 + [HB] * 3 + [VM],
        [vm((8, toks), f32), vm((nt, 8, toks), f32), DMA((nt,)), DMA((nt,))] + [DMA((2, n))] * 6 + [DMA((3,))],
        (q_raw, k_raw, v, cosine, sine, q_gain, k_gain, wo))


def enter_kernel(n, nt, part, hidden, gain, dy, coef, n2_all, h1, dy_all, coef_all,
                 zgot, n2, zs, zr, ps, pr, gs, gr, ys, yr, cs, cr, loc):
    d, t = lax.axis_index("dp"), lax.axis_index("tensor")
    greet(n, nt, d, t)
    z = ZSum(nt, t, part, zgot, zs, zr)
    z.start()
    gy = Gather(n, d, dy, lambda o: dy_all.at[o], ys, yr)
    gc = Gather(n, d, coef, lambda o: coef_all.at[o], cs, cr)
    gc.start()
    gy.start()
    own_y = pltpu.make_async_copy(dy, dy_all.at[d], loc.at[0])
    own_c = pltpu.make_async_copy(coef, coef_all.at[d], loc.at[1])
    own_y.start()
    own_c.start()
    value = hidden[pl.ds(t * z.share, z.share), :].astype(f32) + z.total()
    h1[...] = value
    n2[...] = (value * inv_rms(value) * gain[...]).astype(bf16)
    s = Spread(n, nt, d, t, n2, n2_all, ps, pr, gs, gr)
    own_n = pltpu.make_async_copy(n2, n2_all.at[d, t], loc.at[2])
    s.start()
    own_n.start()
    for j in range(len(bit_list(n))):
        gc.stage(j)
        gy.stage(j)
    s.run()
    s.finish()
    gy.finish()
    gc.finish()
    z.finish()
    own_y.wait()
    own_c.wait()
    own_n.wait()


def enter(n, nt, part, hidden, gain, dy, coef, cid):
    rows, cols = part.shape
    share = rows // nt
    sds = jax.ShapeDtypeStruct
    return kernel_call(
        functools.partial(enter_kernel, n, nt), "enter", cid, [VM, VM, VM, HB, HB],
        [sds((n, nt, share, cols), bf16), sds((share, cols), f32), sds((n,) + dy.shape, dy.dtype), sds((n,) + coef.shape, coef.dtype)],
        [HB, VM, HB, HB],
        [pltpu.VMEM((nt, share, cols), bf16), pltpu.VMEM((share, cols), bf16), DMA((nt,)), DMA((nt,)), DMA((nt,)), DMA((nt,)),
         DMA((nt, 2, n)), DMA((nt, 2, n)), DMA((2, n)), DMA((2, n)), DMA((2, n)), DMA((2, n)), DMA((3,))],
        (part, hidden, gain, dy, coef))


def leave_kernel(n, nt, both, *refs):
    if both:
        (dn2, h1, cot, gain, q, o, moe, dh1, dh1r_all, gain_part, q_all, o_all, moe_part,
         got, got2, part, zgot, low, ss, rs, ss2, rs2, zs, zr, xs, xr, qs, qr, os, orr, loc) = refs
    else:
        (dn2, h1, cot, gain, q, o, dh1, dh1r_all, gain_part, q_all, o_all,
         got, part, zgot, low, ss, rs, zs, zr, xs, xr, qs, qr, os, orr, loc) = refs
    d, t = lax.axis_index("dp"), lax.axis_index("tensor")
    greet(n, nt, d, t)
    steps = len(bit_list(n))

    def put(rows, total):
        part[rows, :] = total.astype(bf16)

    a = Reduce(n, d, dn2, got, ss, rs)
    z = ZSum(nt, t, part, zgot, zs, zr)
    if both:
        b = Reduce(n, d, moe, got2, ss2, rs2)

        def put2(rows, total):
            moe_part[rows, :] = total.astype(bf16)

    a.send(0)
    gathers = [Gather(n, d, q, lambda i: q_all.at[i], qs, qr), Gather(n, d, o, lambda i: o_all.at[i], os, orr)]
    own = [pltpu.make_async_copy(q, q_all.at[d], loc.at[0]), pltpu.make_async_copy(o, o_all.at[d], loc.at[1])]
    for g in gathers:
        g.start()
    for c in own:
        c.start()
    a.recv(0, put)
    for j in range(1, steps):
        a.send(j)
        if both and j == 1:
            b.send(0)
        a.recv(j, put)
    z.start()
    if both:
        b.recv(0, put2)
        b.send(1)
    value = h1[...]
    dz = z.total()
    r = inv_rms(value)
    weighted = dz * gain[...]
    grad = r * weighted - value * (r * r * r) * jnp.mean(weighted * value, axis=-1, keepdims=True)
    grad = cot[pl.ds(t * z.share, z.share), :].astype(f32) + grad
    dh1[...] = grad
    low[...] = grad.astype(bf16)
    dh1r_all[t] = grad.astype(bf16)
    gain_part[...] = jnp.broadcast_to(jnp.sum(dz * value * r, axis=0, keepdims=True), gain_part.shape)
    x = Direct("tensor", nt, t, low, dh1r_all, xs, xr)
    x.start()
    for j in range(steps):
        for g in gathers:
            g.stage(j)
    if both:
        for j in range(1, steps):
            b.recv(j, put2)
            if j + 1 < steps:
                b.send(j + 1)
        b.finish()
    x.wait()
    for e in (a, z, x, *gathers):
        e.finish()
    for c in own:
        c.wait()


def leave(n, nt, dn2, moe, h1, cot, gain, q, o, cid):
    _, rows, cols = dn2.shape
    share = rows // nt
    sds, vm = jax.ShapeDtypeStruct, pltpu.VMEM
    both = moe is not None
    outs = [sds((share, cols), f32), sds((nt, share, cols), bf16), sds((8, cols), f32)] + [sds((n,) + q.shape, bf16)] * 2
    if both:
        outs.append(sds((rows, cols), bf16))
    got = [vm((2, n, rows // 2, cols), bf16)] * (2 if both else 1)
    sems = [DMA((2, n))] * (4 if both else 2) + [DMA((nt,))] * 4 + [DMA((2, n))] * 4 + [DMA((2,))]
    args = (dn2, h1, cot, gain, q, o) + ((moe,) if both else ())
    return kernel_call(
        functools.partial(leave_kernel, n, nt, both), "leave", cid, [VM] * 4 + [HB] * 2 + [VM] * both, outs, [VM] * 3 + [HB] * 2 + [VM] * both,
        got + [vm((rows, cols), bf16), vm((nt, share, cols), bf16), vm((share, cols), bf16)] + sems, args)


def fold_kernel(n, nt, p, out, got, ss, rs):
    d = lax.axis_index("dp")
    hello(dp_peers(n, d))

    def put(rows, total):
        out[rows, :] = total.astype(bf16)

    a = Reduce(n, d, p, got, ss, rs)
    for j in range(len(bit_list(n))):
        a.send(j)
        a.recv(j, put)
    a.finish()


def fold(n, nt, p, cid):
    _, rows, cols = p.shape
    return kernel_call(functools.partial(fold_kernel, n, nt), "fold", cid, [VM], jax.ShapeDtypeStruct((rows, cols), bf16), VM,
                       [pltpu.VMEM((2, n, rows // 2, cols), bf16), DMA((2, n)), DMA((2, n))], (p,))


def back_kernel(n, nt, count, *refs):
    moe, h1, slices, srcs = *refs[:3], refs[3:3 + count]
    out_all, slices_all, dsts = *refs[3 + count:5 + count], refs[5 + count:5 + 2 * count]
    zgot, low, zs, zr, xs, xr, gs, gr, bs, br, loc = refs[5 + 2 * count:]
    d, t = lax.axis_index("dp"), lax.axis_index("tensor")
    greet(n, nt, d, t, True)
    z = ZSum(nt, t, moe, zgot, zs, zr)
    gathers = [Gather(n, d, srcs[i], (lambda o, i=i: dsts[i].at[o]), gs.at[i], gr.at[i]) for i in range(count)]
    own = [pltpu.make_async_copy(srcs[i], dsts[i].at[d], loc.at[i]) for i in range(count)]
    own.append(pltpu.make_async_copy(slices.at[d], slices_all.at[d], loc.at[count]))
    for g in gathers:
        g.start()
    z.start()
    b = Direct("dp", n, d, slices, slices_all, bs, br, True)
    b.start()
    for c in own:
        c.start()
    for g in gathers:
        g.stage(0)
    value = (h1[...] + z.total()).astype(bf16)
    low[...] = value
    out_all[t] = value
    x = Direct("tensor", nt, t, low, out_all, xs, xr)
    x.start()
    for j in range(1, len(bit_list(n))):
        for g in gathers:
            g.stage(j)
    x.wait()
    b.wait()
    for g in gathers:
        g.finish()
    for c in own:
        c.wait()
    for e in (z, x, b):
        e.finish()


def back(n, nt, moe, h1, slices, arrs, cid):
    rows, cols = moe.shape
    share = rows // nt
    sds = jax.ShapeDtypeStruct
    k = len(arrs)
    return kernel_call(
        functools.partial(back_kernel, n, nt, k), "back", cid, [VM, VM] + [HB] * (k + 1),
        [sds((nt, share, cols), bf16), sds(slices.shape, bf16)] + [sds((n,) + a.shape, a.dtype) for a in arrs], [VM] + [HB] * (k + 1),
        [pltpu.VMEM((nt, share, cols), bf16), pltpu.VMEM((share, cols), bf16)] + [DMA((nt,))] * 4 + [DMA((k, 2, n))] * 2 + [DMA((n,))] * 2 + [DMA((k + 1,))],
        (moe, h1, slices, *arrs))


def last_kernel(n, nt, count, *refs):
    dnormed, hidden, gain, dh1, gains, srcs = *refs[:5], refs[5:5 + count]
    grad_all, gains_out, dsts = *refs[5 + count:7 + count], refs[7 + count:7 + 2 * count]
    (zgot, low, gpart, ggot, gsum, gall, zs, zr, xs, xr, gs, gr, ps, pr, qs, qr, loc) = refs[7 + 2 * count:]
    d, t = lax.axis_index("dp"), lax.axis_index("tensor")
    greet(n, nt, d, t, True)
    z = ZSum(nt, t, dnormed, zgot, zs, zr)
    z.start()
    gathers = [Gather(n, d, srcs[i], (lambda o, i=i: dsts[i].at[o]), gs.at[i], gr.at[i]) for i in range(count)]
    own = [pltpu.make_async_copy(srcs[i], dsts[i].at[d], loc.at[i]) for i in range(count)]
    for g in gathers:
        g.start()
    for c in own:
        c.start()
    for g in gathers:
        g.stage(0)
    dz = z.total()
    value = hidden[pl.ds(t * z.share, z.share), :].astype(f32)
    r = inv_rms(value)
    weighted = dz * gain[...]
    grad = r * weighted - value * (r * r * r) * jnp.mean(weighted * value, axis=-1, keepdims=True)
    grad = (dh1[...] + grad).astype(bf16)
    low[...] = grad
    grad_all[t] = grad
    x = Direct("tensor", nt, t, low, grad_all, xs, xr)
    x.start()
    row = jnp.sum(dz * value * r, axis=0, keepdims=True)
    first = lax.broadcasted_iota(jnp.int32, gains.shape, 0) == 0
    whole = jnp.where(first, row, gains[...])
    width = gpart.shape[2]
    for i in range(n):
        gpart[i] = whole[:, i * width:(i + 1) * width]
    p = Direct("dp", n, d, gpart, ggot, ps, pr, True)
    p.start()
    for j in range(1, len(bit_list(n))):
        for g in gathers:
            g.stage(j)
    p.wait()
    total = gpart[d]
    for m in range(1, n):
        total = total + ggot[flip(d, m)]
    gsum[...] = total
    gall[t] = total
    q = Direct("tensor", nt, t, gsum, gall, qs, qr)
    q.start()
    x.wait()
    q.wait()
    total = gall[0]
    for i in range(1, nt):
        total = total + gall[i]
    gains_out[...] = total
    for g in gathers:
        g.finish()
    for c in own:
        c.wait()
    for e in (z, x, p, q):
        e.finish()


def last(n, nt, dnormed, hidden, gain, dh1, gains, arrs, cid):
    rows, cols = dnormed.shape
    share = rows // nt
    width = cols // n
    sds, vm = jax.ShapeDtypeStruct, pltpu.VMEM
    k = len(arrs)
    return kernel_call(
        functools.partial(last_kernel, n, nt, k), "last", cid, [VM] * 5 + [HB] * k,
        [sds((nt, share, cols), bf16), sds((8, width), f32)] + [sds((n,) + a.shape, a.dtype) for a in arrs],
        [VM, VM] + [HB] * k,
        [vm((nt, share, cols), bf16), vm((share, cols), bf16), vm((n, 8, width), f32), vm((n, 8, width), f32), vm((8, width), f32),
         vm((nt, 8, width), f32)] + [DMA((nt,))] * 4 + [DMA((k, 2, n))] * 2 + [DMA((n,))] * 2 + [DMA((nt,))] * 2 + [DMA((k,))],
        (dnormed, hidden, gain, dh1, gains, *arrs))


def weight_grad_kernel(order, a_ref, b_ref, out_ref):
    per = b_ref.shape[2] // 128
    for i in range(b_ref.shape[0]):
        res = contract(a_ref[...], b_ref[i], 0, 0)
        for f in range(per):
            out_ref[pl.ds(order[i * per + f], res.shape[0], stride=len(order)), :] = res[:, f * 128:(f + 1) * 128]


def weight_grad(a, b, order):
    toks, rows = a.shape
    block = 256
    return pl.pallas_call(
        functools.partial(weight_grad_kernel, order),
        grid=(rows // block,),
        in_specs=[pl.BlockSpec((toks, block), lambda i: (0, i)), pl.BlockSpec(b.shape, lambda i: (0, 0, 0))],
        out_specs=pl.BlockSpec((block * len(order), 128), lambda i: (i, 0)),
        out_shape=jax.ShapeDtypeStruct((rows * len(order), 128), f32),
        name="weight_grad",
    )(a, b)


def direct_kernel(axis, n, split, count, *refs):
    srcs, dsts, ss, rs, loc = refs[:count], refs[count:2 * count], *refs[2 * count:]
    me = lax.axis_index(axis)
    own = [pltpu.make_async_copy(srcs[i].at[me] if split else srcs[i], dsts[i].at[me], loc.at[i]) for i in range(count)]
    hello(all_peers(axis, n, me))
    sent = []
    for m in range(1, n):
        for i in range(count):
            peer = flip(me, m)
            c = rdma(srcs[i].at[peer] if split else srcs[i], dsts[i].at[me], ss.at[i, m], rs.at[i, m], {axis: peer})
            c.start()
            sent.append(c)
    for c in own:
        c.start()
    for m in range(1, n):
        for i in range(count):
            place = dsts[i].at[flip(me, m)]
            rdma(place, place, ss.at[i, m], rs.at[i, m], {axis: flip(me, m)}).wait_recv()
    for c in sent:
        c.wait_send()
    for c in own:
        c.wait()


def direct(axis, n, arrs, cid, split=False):
    arrs = list(arrs)
    scratch = [pltpu.SemaphoreType.DMA((len(arrs), n))] * 2 + [pltpu.SemaphoreType.DMA((len(arrs),))]
    outs = [jax.ShapeDtypeStruct(a.shape if split else (n,) + a.shape, a.dtype) for a in arrs]
    return call(functools.partial(direct_kernel, axis, n, split, len(arrs)), "direct_" + axis, cid, outs, pltpu.VMEM, pltpu.VMEM, scratch, *arrs)


D = 2048
HD = 128
TOPK = 8
EPSILON = 1e-05
ROPE_BASE = 10000.0
NEG_FILL = -1e30


def norm_back(values, gain, grad_out):
    inv_rms = lax.rsqrt(jnp.mean(values * values, axis=-1, keepdims=True) + EPSILON)
    weighted = grad_out * gain
    grad_in = inv_rms * weighted - values * inv_rms**3 * jnp.mean(weighted * values, axis=-1, keepdims=True)
    return grad_in, jnp.sum(grad_out * values * inv_rms, axis=0)


def locate(anchor, lengths):
    ends = jnp.cumsum(lengths)
    starts = ends - lengths
    docs = jnp.sum((anchor[:, None] >= ends[None, :]).astype(jnp.int32), axis=1)
    which = docs[:, None] == jnp.arange(lengths.shape[0], dtype=jnp.int32)[None, :]
    begins = jnp.sum(jnp.where(which, starts[None, :], 0), axis=1)
    return docs, (anchor - begins).astype(jnp.int32)


def rope_tables(positions):
    half_dim = HD // 2
    freqs = ROPE_BASE ** (-2.0 * jnp.arange(half_dim, dtype=f32) / HD)
    angles = positions.astype(f32)[:, None] * freqs[None, :]
    cosine, sine = jnp.cos(angles), jnp.sin(angles)
    return jnp.concatenate([cosine, cosine], axis=1)[:, None, :], jnp.concatenate([-sine, sine], axis=1)[:, None, :]


def turn(x, cosine, sine):
    return x * cosine + jnp.roll(x, HD // 2, axis=-1) * sine


def pair_allowed(query_anchor, query_docs, key_anchor, key_docs):
    return ((query_docs[:, None] == key_docs[None, :]) & (key_anchor[None, :] <= query_anchor[:, None]))[None]


def contract(left, right, l, r):
    return lax.dot_general(left, right, (((l,), (r,)), ((), ())), preferred_element_type=f32)


def routing(experts, gates, num_exp, capacity):
    toks = experts.shape[0]
    chosen = experts[:, :, None] == jnp.arange(num_exp, dtype=jnp.int32)[None, None, :]
    mask = jnp.any(chosen, axis=1)
    gate = jnp.sum(jnp.where(chosen, gates[:, :, None], 0.0), axis=1)
    index = jnp.arange(toks, dtype=jnp.int32)
    before = (index[:, None] > index[None, :]).astype(bf16)
    slot = contract(before, mask.astype(bf16), 1, 0)
    return jnp.where(mask & (slot < capacity), gate, 0.0)


def small(rows):
    rows = jnp.stack(rows)
    return jnp.pad(rows, ((0, -rows.shape[0] % 8), (0, 0)))


def shards(hidden_in, attn_gain, query_weight, key_weight, value_weight, output_weight, query_gain, key_gain,
           moe_gain, expert_gate_up, expert_down, experts, gates, anchor, lengths, cotangent):
    n, nt = lax.axis_size("dp"), lax.axis_size("tensor")
    d, t = lax.axis_index("dp"), lax.axis_index("tensor")
    toks = hidden_in.shape[0]
    share = toks // nt
    cols = query_weight.shape[1]
    heads = cols // HD
    scale = HD ** (-0.5)
    exp_local = expert_down.shape[1]
    num_exp = exp_local * n
    capacity = 9 * toks * TOPK // (8 * num_exp)
    hidden = hidden_in.astype(f32)

    def mine(a):
        return lax.dynamic_slice_in_dim(a, t * share, share, 0)

    coef = routing(experts, gates, num_exp, capacity).T
    place = jnp.broadcast_to(anchor[None, :], (16, toks))
    wq, wk, wv, anchor_all = gather_dp(n, (query_weight, key_weight, value_weight, place), 1)
    wq, wk, wv = (w.reshape(D, cols) for w in (wq, wk, wv))
    anchor_all = anchor_all[:, 0].reshape(n * toks)

    docs, positions = locate(anchor, lengths)
    docs_all, _ = locate(anchor_all, lengths)
    cosine, sine = rope_tables(positions)
    allowed = pair_allowed(anchor, docs, anchor_all, docs_all)
    allowed_back = pair_allowed(anchor_all, docs_all, anchor, docs)

    inv = lax.rsqrt(jnp.mean(hidden * hidden, axis=-1, keepdims=True) + EPSILON)
    normed = (hidden * inv * attn_gain).astype(bf16)
    q_raw, k_raw, v_raw = (contract(normed, w, 1, 0) for w in (wq, wk, wv))
    v = v_raw.astype(bf16)
    q, k, k_all, v_all, wo, sq = mix(
        n, nt, q_raw, k_raw, v, cosine[:, 0], sine[:, 0], query_gain[None, :], key_gain[None, :], output_weight, 2)
    wo = wo.reshape(D, cols)
    q_inv = lax.rsqrt(sq[0] / D + EPSILON)[:, None]
    k_inv = lax.rsqrt(sq[1] / D + EPSILON)[:, None]
    q_flat = q
    q, k, v = (a.reshape(toks, heads, HD) for a in (q, k, v))
    k_all, v_all = (a.reshape(n * toks, heads, HD) for a in (k_all, v_all))

    scores = scale * jnp.einsum("qhd,khd->hqk", q, k_all, preferred_element_type=f32)
    top = jnp.max(jnp.where(allowed, scores, NEG_FILL), axis=2)
    probs = jnp.where(allowed, jnp.exp(scores - top[:, :, None]), 0.0)
    total = jnp.sum(probs, axis=2)
    lse = top + jnp.log(total)
    attended = jnp.einsum("hqk,khd->qhd", probs.astype(bf16), v_all, preferred_element_type=f32)
    attended = attended / total.T[:, :, None]
    o = attended.reshape(toks, cols).astype(bf16)
    n2_all, h1, dy_all, coef_all = enter(
        n, nt, contract(o, wo, 1, 1).astype(bf16), hidden_in, moe_gain[None, :], cotangent, coef, 4)
    n2_all, dy_all = n2_all.reshape(n * toks, D), dy_all.reshape(n * toks, D)
    coef_all = lax.dynamic_slice_in_dim(coef_all, d * exp_local, exp_local, 1)
    coef_all = coef_all.transpose(1, 0, 2).reshape(exp_local, n * toks, 1)

    gu = jnp.einsum("td,dezf->eztf", n2_all, expert_gate_up, preferred_element_type=f32)
    g, u = gu[:, 0], gu[:, 1]
    sig = jax.nn.sigmoid(g)
    act = (coef_all * (g * sig * u)).astype(bf16)
    dact = coef_all * jnp.einsum("td,def->etf", dy_all, expert_down, preferred_element_type=f32)
    dgu = jnp.stack([dact * u * sig * (1.0 + g * (1.0 - sig)), dact * (g * sig)], axis=1).astype(bf16)
    act, dgu = lax.optimization_barrier((act, dgu))
    dn2 = jnp.einsum("eztf,dezf->td", dgu, expert_gate_up, preferred_element_type=f32).astype(bf16)
    moe = jnp.einsum("etf,def->td", act, expert_down, preferred_element_type=f32).astype(bf16)
    half = expert_down.shape[2] // 128
    down_grad = weight_grad(dy_all, act, [f * exp_local + e for e in range(exp_local) for f in range(half)])
    down_grad = down_grad.reshape(D, half, exp_local, 128).transpose(0, 2, 1, 3).reshape(expert_down.shape)
    gate_up_grad = weight_grad(n2_all, dgu.reshape(2 * exp_local, n * toks, -1),
                               [(e * half + f) * 2 + z for e in range(exp_local) for z in (0, 1) for f in range(half)])
    gate_up_grad = gate_up_grad.reshape(D, exp_local, half, 2, 128).transpose(0, 1, 3, 2, 4).reshape(expert_gate_up.shape)

    dn2, moe = dn2.reshape(n, toks, D), moe.reshape(n, toks, D)
    together = 16 * n * toks * D <= 48 * 2**20
    dh1, dh1r, moe_gain_part, q_all, o_all, *rest = leave(
        n, nt, dn2, moe if together else None, h1, cotangent, moe_gain[None, :], q_flat, o, 6)
    moe = rest[0] if together else fold(n, nt, moe, 7)
    dh1r = dh1r.reshape(toks, D)

    do = contract(dh1r, wo, 1, 0).astype(bf16)
    delta = jnp.sum(do.reshape(toks, heads, HD).astype(f32) * attended, axis=2).T
    terms = small(list(lse) + list(delta))
    if terms.shape[0] % 16:
        terms = jnp.pad(terms, ((0, 8), (0, 0)))
    slices = jnp.concatenate([normed, dh1r], axis=0).reshape(2 * toks, n, D // n).transpose(1, 0, 2)
    output, slices, do_all, stats_all = back(n, nt, moe, h1, slices, (do, terms), 9)
    output = output.reshape(toks, D)

    do = do.reshape(toks, heads, HD)
    q_all, do_all = (a.reshape(n * toks, heads, HD) for a in (q_all, do_all))
    lse_all = stats_all[:, :heads].transpose(1, 0, 2).reshape(heads, n * toks)
    delta_all = stats_all[:, heads:2 * heads].transpose(1, 0, 2).reshape(heads, n * toks)
    probs = jnp.where(allowed, jnp.exp(scores - lse[:, :, None]), 0.0)
    dprobs = jnp.einsum("qhd,khd->hqk", do, v_all, preferred_element_type=f32)
    ds = (probs * (dprobs - delta[:, :, None])).astype(bf16)
    dq = scale * jnp.einsum("hqk,khd->qhd", ds, k_all, preferred_element_type=f32)
    scores_b = scale * jnp.einsum("qhd,khd->hqk", q_all, k, preferred_element_type=f32)
    probs_b = jnp.where(allowed_back, jnp.exp(scores_b - lse_all[:, :, None]), 0.0)
    dv = jnp.einsum("hqk,qhd->khd", probs_b.astype(bf16), do_all, preferred_element_type=f32)
    dprobs_b = jnp.einsum("qhd,khd->hqk", do_all, v, preferred_element_type=f32)
    ds_b = (probs_b * (dprobs_b - delta_all[:, :, None])).astype(bf16)
    dk = scale * jnp.einsum("hqk,qhd->khd", ds_b, q_all, preferred_element_type=f32)
    dq_hat = turn(dq, cosine, -sine).reshape(toks, cols)
    dk_hat = turn(dk, cosine, -sine).reshape(toks, cols)
    dv = dv.reshape(toks, cols).astype(bf16)

    wdq, wdk = dq_hat * query_gain, dk_hat * key_gain
    q_gain_part = jnp.sum(dq_hat * q_raw * q_inv, axis=0)
    k_gain_part = jnp.sum(dk_hat * k_raw * k_inv, axis=0)
    (cross,) = direct("tensor", nt, [small([jnp.sum(wdq * q_raw, axis=1), jnp.sum(wdk * k_raw, axis=1)])], 11)
    cross = jnp.sum(cross, axis=0)
    dq_raw = (q_inv * wdq - q_raw * q_inv**3 * cross[0][:, None] / D).astype(bf16)
    dk_raw = (k_inv * wdk - k_raw * k_inv**3 * cross[1][:, None] / D).astype(bf16)
    dnormed = contract(dq_raw, wq, 1, 1) + contract(dk_raw, wk, 1, 1) + contract(dv, wv, 1, 1)

    def wide(part):
        return lax.dynamic_update_slice_in_dim(jnp.zeros((D,), f32), part, t * cols, 0)

    gains = small([jnp.zeros((D,), f32), wide(q_gain_part), wide(k_gain_part), moe_gain_part[0]])
    input_grad, gains, dq_all, dk_all, dv_all = last(
        n, nt, dnormed.astype(bf16), hidden_in, attn_gain[None, :], dh1, gains, (dq_raw, dk_raw, dv), 12)
    normed_all = slices[:, :toks].reshape(n * toks, D // n)
    dh1r_all = slices[:, toks:].reshape(n * toks, D // n)
    output_grad = contract(dh1r_all, o_all.reshape(n * toks, cols), 0, 0)
    query_grad, key_grad, value_grad = (
        contract(normed_all, a.reshape(n * toks, cols), 0, 0) for a in (dq_all, dk_all, dv_all))
    input_grad = input_grad.reshape(toks, D).astype(f32)
    return (output, input_grad, query_grad, key_grad, value_grad, output_grad, gate_up_grad, down_grad,
            gains[0], gains[1], gains[2], gains[3])


def solution(mesh):
    in_specs = (
        P("dp", None),
        P(),
        P("dp", "tensor"),
        P("dp", "tensor"),
        P("dp", "tensor"),
        P("dp", "tensor"),
        P("tensor"),
        P("tensor"),
        P(),
        P(None, "dp", None, "tensor"),
        P(None, "dp", "tensor"),
        P("dp", None),
        P("dp", None),
        P("dp"),
        P(),
        P("dp", None),
    )
    out_specs = (
        P("dp", None),
        P("dp", None),
        P("dp", "tensor"),
        P("dp", "tensor"),
        P("dp", "tensor"),
        P("dp", "tensor"),
        P(None, "dp", None, "tensor"),
        P(None, "dp", "tensor"),
        P("dp"),
        P("dp"),
        P("dp"),
        P("dp"),
    )
    return jax.shard_map(shards, mesh=mesh, in_specs=in_specs, out_specs=out_specs, check_vma=False)
```

```python
import functools
import jax
import jax.numpy as jnp
from jax import lax
from jax.experimental import pallas as pl
from jax.experimental.pallas import tpu as pltpu
from jax.sharding import PartitionSpec as P

MESH = pl.DeviceIdType.MESH
f32 = jnp.float32
bf16 = jnp.bfloat16


def bit_list(n):
    bits, b = [], 1
    while b < n:
        bits.append(b)
        b *= 2
    return bits


def flip(i, m):
    for b in bit_list(m + 1):
        if m & b:
            i = i + b - 2 * b * ((i // b) % 2)
    return i


def span(bits):
    out = [0]
    for b in bits:
        out = out + [m | b for m in out]
    return out


def orders(n):
    bits = bit_list(n)
    outer = bits[1:]
    return (outer + bits[:1], outer[::-1] + bits[:1])


def hello(peers):
    barrier = pltpu.get_barrier_semaphore()
    for peer in peers:
        pl.semaphore_signal(barrier, inc=1, device_id=peer, device_id_type=MESH)
    pl.semaphore_wait(barrier, len(peers))


def rdma(src, dst, send_sem, recv_sem, peer):
    return pltpu.make_async_remote_copy(
        src_ref=src, dst_ref=dst, send_sem=send_sem, recv_sem=recv_sem,
        device_id=peer, device_id_type=MESH,
    )


class Gather:
    def __init__(self, n, me, src, dst, send_sems, recv_sems):
        self.n, self.me, self.src, self.dst = n, me, src, dst
        self.send_sems, self.recv_sems = send_sems, recv_sems
        self.half = src.shape[0] // 2
        self.sent = []

    def push(self, h, m, bit):
        rows = pl.ds(h * self.half, self.half)
        place = self.dst(flip(self.me, m)).at[rows]
        copy = rdma(self.src.at[rows] if m == 0 else place, place, self.send_sems.at[h, m | bit],
                    self.recv_sems.at[h, m | bit], {"dp": flip(self.me, bit)})
        copy.start()
        self.sent.append(copy)

    def start(self):
        o = orders(self.n)
        for j in range(len(o[0])):
            for h in (0, 1):
                self.push(h, 0, o[h][j])

    def stage(self, j):
        o = orders(self.n)
        for i in range(2**j):
            for h in (0, 1):
                m = span(o[h][:j])[i] | o[h][j]
                place = self.dst(flip(self.me, m)).at[pl.ds(h * self.half, self.half)]
                rdma(place, place, self.send_sems.at[h, m], self.recv_sems.at[h, m],
                     {"dp": flip(self.me, o[h][j])}).wait_recv()
                for bit in o[h][j + 1:]:
                    self.push(h, m, bit)

    def finish(self):
        for copy in self.sent:
            copy.wait_send()


def dp_peers(n, me):
    return [{"dp": flip(me, b)} for b in bit_list(n)]


def all_peers(axis, n, me):
    return [{axis: flip(me, m)} for m in range(1, n)]


def call(kernel, name, cid, outs, out_space, in_space, scratch, *args):
    single = not isinstance(outs, (list, tuple))
    spec = pl.BlockSpec(memory_space=out_space)
    return pl.pallas_call(
        kernel,
        out_shape=outs,
        in_specs=[pl.BlockSpec(memory_space=in_space)] * len(args),
        out_specs=spec if single else [spec] * len(outs),
        scratch_shapes=scratch,
        compiler_params=pltpu.CompilerParams(collective_id=cid, has_side_effects=True),
        name=name,
    )(*args)


def gather_kernel(n, count, *refs):
    srcs, dsts, sems = refs[:count], refs[count:2 * count], refs[2 * count:]
    me = lax.axis_index("dp")
    own = [pltpu.make_async_copy(srcs[i], dsts[i].at[me], sems[2 * count].at[i]) for i in range(count)]
    hello(dp_peers(n, me))
    gathers = [Gather(n, me, srcs[i], (lambda o, i=i: dsts[i].at[o]), sems[2 * i], sems[2 * i + 1]) for i in range(count)]
    for g in gathers:
        g.start()
    for c in own:
        c.start()
    for j in range(len(bit_list(n))):
        for g in gathers:
            g.stage(j)
    for g in gathers:
        g.finish()
    for c in own:
        c.wait()


def gather_dp(n, arrs, cid):
    arrs = list(arrs)
    scratch = [pltpu.SemaphoreType.DMA((2, n))] * (2 * len(arrs)) + [pltpu.SemaphoreType.DMA((len(arrs),))]
    outs = [jax.ShapeDtypeStruct((n,) + a.shape, a.dtype) for a in arrs]
    return call(functools.partial(gather_kernel, n, len(arrs)), "gather_dp", cid, outs, pl.ANY, pl.ANY, scratch, *arrs)


class Spread:
    def __init__(self, n, nt, d, t, src, dst, zs, zr, gs, gr):
        self.nt, self.t, self.d, self.src, self.dst, self.zs, self.zr = nt, t, d, src, dst, zs, zr
        self.steps = len(bit_list(n))
        self.gathers = []
        for m in range(nt):
            tm = flip(t, m)
            own = src if m == 0 else dst.at[d, tm]
            self.gathers.append(Gather(n, d, own, (lambda o, tm=tm: dst.at[o, tm]), gs.at[m], gr.at[m]))
        self.sent = []

    def start(self):
        for m in range(1, self.nt):
            c = rdma(self.src, self.dst.at[self.d, self.t], self.zs.at[m], self.zr.at[m], {"tensor": flip(self.t, m)})
            c.start()
            self.sent.append(c)
        self.gathers[0].start()

    def run(self):
        done = [0] * self.nt
        for m in range(1, self.nt):
            place = self.dst.at[self.d, flip(self.t, m)]
            rdma(place, place, self.zs.at[m], self.zr.at[m], {"tensor": flip(self.t, m)}).wait_recv()
            self.gathers[m].start()
            for k in range(m):
                if done[k] < self.steps and k + done[k] < m:
                    self.gathers[k].stage(done[k])
                    done[k] += 1
        for j in range(self.steps):
            for m in range(self.nt):
                if done[m] == j:
                    self.gathers[m].stage(j)
                    done[m] = j + 1

    def finish(self):
        for g in self.gathers:
            g.finish()
        for c in self.sent:
            c.wait_send()


class Reduce:
    def __init__(self, n, me, p, got, send_sems, recv_sems):
        self.n, self.me, self.p, self.got, self.ss, self.rs = n, me, p, got, send_sems, recv_sems
        self.half = p.shape[1] // 2
        self.bits = len(bit_list(n))
        self.o = [x[::-1] for x in orders(n)]
        self.keeps = [[span(self.o[h][j + 1:]) for h in (0, 1)] for j in range(self.bits)]
        self.base = [sum(len(self.keeps[k][0]) for k in range(j)) for j in range(self.bits)]
        self.sent = []

    def piece(self, j, h, m):
        if j == 0:
            return self.p.at[flip(self.me, m), pl.ds(h * self.half, self.half)]
        return self.got.at[h, self.base[j - 1] + self.keeps[j - 1][h].index(m)]

    def each(self, j):
        for i in range(len(self.keeps[j][0])):
            for h in (0, 1):
                yield h, self.keeps[j][h][i], self.o[h][j], self.base[j] + i

    def send(self, j):
        for h, m, b, k in self.each(j):
            c = rdma(self.piece(j, h, m | b), self.got.at[h, k], self.ss.at[h, k], self.rs.at[h, k], {"dp": flip(self.me, b)})
            c.start()
            self.sent.append(c)

    def recv(self, j, put=None):
        for h, m, b, k in self.each(j):
            view = self.got.at[h, k]
            rdma(view, view, self.ss.at[h, k], self.rs.at[h, k], {"dp": flip(self.me, b)}).wait_recv()
            total = self.piece(j, h, m)[...].astype(f32) + view[...].astype(f32)
            if j == self.bits - 1:
                put(pl.ds(h * self.half, self.half), total)
            else:
                view[...] = total.astype(bf16)

    def finish(self):
        for c in self.sent:
            c.wait_send()


class ZSum:
    def __init__(self, nt, t, src, got, zs, zr):
        self.nt, self.t, self.src, self.got, self.zs, self.zr = nt, t, src, got, zs, zr
        self.share = src.shape[0] // nt
        self.sent = []

    def start(self):
        for m in range(1, self.nt):
            peer = flip(self.t, m)
            c = rdma(self.src.at[pl.ds(peer * self.share, self.share)], self.got.at[m], self.zs.at[m], self.zr.at[m], {"tensor": peer})
            c.start()
            self.sent.append(c)

    def total(self):
        total = self.src[pl.ds(self.t * self.share, self.share), :].astype(f32)
        for m in range(1, self.nt):
            v = self.got.at[m]
            rdma(v, v, self.zs.at[m], self.zr.at[m], {"tensor": flip(self.t, m)}).wait_recv()
            total = total + v[...].astype(f32)
        return total

    def finish(self):
        for c in self.sent:
            c.wait_send()


class Direct:
    def __init__(self, axis, n, me, src, dst, ss, rs, split=False):
        self.axis, self.n, self.me, self.src, self.dst, self.ss, self.rs, self.split = axis, n, me, src, dst, ss, rs, split
        self.sent = []

    def start(self):
        for m in range(1, self.n):
            peer = flip(self.me, m)
            c = rdma(self.src.at[peer] if self.split else self.src, self.dst.at[self.me], self.ss.at[m], self.rs.at[m], {self.axis: peer})
            c.start()
            self.sent.append(c)

    def wait(self):
        for m in range(1, self.n):
            place = self.dst.at[flip(self.me, m)]
            rdma(place, place, self.ss.at[m], self.rs.at[m], {self.axis: flip(self.me, m)}).wait_recv()

    def finish(self):
        for c in self.sent:
            c.wait_send()


def greet(n, nt, d, t, every_dp=False):
    hello((all_peers("dp", n, d) if every_dp else dp_peers(n, d)) + all_peers("tensor", nt, t))


def inv_rms(v):
    return lax.rsqrt(jnp.mean(v * v, axis=-1, keepdims=True) + EPSILON)


VM = pl.BlockSpec(memory_space=pltpu.VMEM)
HB = pl.BlockSpec(memory_space=pl.ANY)
DMA = pltpu.SemaphoreType.DMA


def kernel_call(kernel, name, cid, in_specs, outs, out_specs, scratch, args):
    return pl.pallas_call(
        kernel, out_shape=outs, in_specs=in_specs, out_specs=out_specs, scratch_shapes=scratch,
        compiler_params=pltpu.CompilerParams(collective_id=cid, has_side_effects=True), name=name,
    )(*args)


def across(column, lanes):
    return jnp.transpose(jnp.broadcast_to(column, (column.shape[0], lanes)))


def mix_kernel(n, nt, q_raw, k_raw, v, cosine, sine, q_gain, k_gain, wo, q, k, k_all, v_all, wo_all, sums,
               sq, sq_all, ss, rs, ws, wr, ks, kr, vs, vr, loc):
    d, t = lax.axis_index("dp"), lax.axis_index("tensor")
    greet(n, nt, d, t)
    row = lax.broadcasted_iota(jnp.int32, sq.shape, 0)
    part_q, part_k = (across(jnp.sum(a[...] * a[...], axis=1, keepdims=True), HD)[:8] for a in (q_raw, k_raw))
    part = jnp.where(row == 0, part_q, jnp.where(row == 1, part_k, 0.0))
    sq[...] = part
    sq_all[t] = part
    x = Direct("tensor", nt, t, sq, sq_all, ss, rs)
    x.start()
    gv = Gather(n, d, v, lambda o: v_all.at[o], vs, vr)
    gv.start()
    own = [pltpu.make_async_copy(v, v_all.at[d], loc.at[0]), pltpu.make_async_copy(wo, wo_all.at[d], loc.at[1])]
    for c in own:
        c.start()
    x.wait()
    total = sq_all[0]
    for i in range(1, nt):
        total = total + sq_all[i]
    sums[...] = total
    inv = lax.rsqrt(total / D + EPSILON)
    for i, (raw, gain, out) in enumerate(((k_raw, k_gain, k), (q_raw, q_gain, q))):
        scale = jnp.transpose(jnp.broadcast_to(inv[i ^ 1:(i ^ 1) + 1], (HD, inv.shape[1])))
        for h in range(raw.shape[1] // HD):
            at = slice(h * HD, (h + 1) * HD)
            y = raw[:, at] * scale * gain[:, at]
            out[:, at] = (y * cosine[...] + pltpu.roll(y, HD // 2, 1) * sine[...]).astype(bf16)
        if i == 0:
            gk = Gather(n, d, k, lambda o: k_all.at[o], ks, kr)
            gk.start()
            gw = Gather(n, d, wo, lambda o: wo_all.at[o], ws, wr)
            gw.start()
            own_k = pltpu.make_async_copy(k, k_all.at[d], loc.at[2])
            own_k.start()
    for j in range(len(bit_list(n))):
        for g in (gv, gk, gw):
            g.stage(j)
    for e in (x, gv, gk, gw):
        e.finish()
    for c in own:
        c.wait()
    own_k.wait()


def mix(n, nt, q_raw, k_raw, v, cosine, sine, q_gain, k_gain, wo, cid):
    toks, cols = v.shape
    sds, vm = jax.ShapeDtypeStruct, pltpu.VMEM
    wide = sds((n, toks, cols), bf16)
    return kernel_call(
        functools.partial(mix_kernel, n, nt), "mix", cid, [VM] * 7 + [HB],
        [sds((toks, cols), bf16)] * 2 + [wide, wide, sds((n,) + wo.shape, bf16), sds((8, toks), f32)], [VM] * 2 + [HB] * 3 + [VM],
        [vm((8, toks), f32), vm((nt, 8, toks), f32), DMA((nt,)), DMA((nt,))] + [DMA((2, n))] * 6 + [DMA((3,))],
        (q_raw, k_raw, v, cosine, sine, q_gain, k_gain, wo))


def enter_kernel(n, nt, part, hidden, gain, dy, coef, n2_all, h1, dy_all, coef_all,
                 zgot, n2, zs, zr, ps, pr, gs, gr, ys, yr, cs, cr, loc):
    d, t = lax.axis_index("dp"), lax.axis_index("tensor")
    greet(n, nt, d, t)
    z = ZSum(nt, t, part, zgot, zs, zr)
    z.start()
    gy = Gather(n, d, dy, lambda o: dy_all.at[o], ys, yr)
    gc = Gather(n, d, coef, lambda o: coef_all.at[o], cs, cr)
    gc.start()
    gy.start()
    own_y = pltpu.make_async_copy(dy, dy_all.at[d], loc.at[0])
    own_c = pltpu.make_async_copy(coef, coef_all.at[d], loc.at[1])
    own_y.start()
    own_c.start()
    value = hidden[pl.ds(t * z.share, z.share), :].astype(f32) + z.total()
    h1[...] = value
    n2[...] = (value * inv_rms(value) * gain[...]).astype(bf16)
    s = Spread(n, nt, d, t, n2, n2_all, ps, pr, gs, gr)
    own_n = pltpu.make_async_copy(n2, n2_all.at[d, t], loc.at[2])
    s.start()
    own_n.start()
    for j in range(len(bit_list(n))):
        gc.stage(j)
        gy.stage(j)
    s.run()
    s.finish()
    gy.finish()
    gc.finish()
    z.finish()
    own_y.wait()
    own_c.wait()
    own_n.wait()


def enter(n, nt, part, hidden, gain, dy, coef, cid):
    rows, cols = part.shape
    share = rows // nt
    sds = jax.ShapeDtypeStruct
    return kernel_call(
        functools.partial(enter_kernel, n, nt), "enter", cid, [VM, VM, VM, HB, HB],
        [sds((n, nt, share, cols), bf16), sds((share, cols), f32), sds((n,) + dy.shape, dy.dtype), sds((n,) + coef.shape, coef.dtype)],
        [HB, VM, HB, HB],
        [pltpu.VMEM((nt, share, cols), bf16), pltpu.VMEM((share, cols), bf16), DMA((nt,)), DMA((nt,)), DMA((nt,)), DMA((nt,)),
         DMA((nt, 2, n)), DMA((nt, 2, n)), DMA((2, n)), DMA((2, n)), DMA((2, n)), DMA((2, n)), DMA((3,))],
        (part, hidden, gain, dy, coef))


def leave_kernel(n, nt, both, *refs):
    if both:
        (dn2, h1, cot, gain, q, o, moe, dh1, dh1r_all, gain_part, q_all, o_all, moe_part,
         got, got2, part, zgot, low, ss, rs, ss2, rs2, zs, zr, xs, xr, qs, qr, os, orr, loc) = refs
    else:
        (dn2, h1, cot, gain, q, o, dh1, dh1r_all, gain_part, q_all, o_all,
         got, part, zgot, low, ss, rs, zs, zr, xs, xr, qs, qr, os, orr, loc) = refs
    d, t = lax.axis_index("dp"), lax.axis_index("tensor")
    greet(n, nt, d, t)
    steps = len(bit_list(n))

    def put(rows, total):
        part[rows, :] = total.astype(bf16)

    a = Reduce(n, d, dn2, got, ss, rs)
    z = ZSum(nt, t, part, zgot, zs, zr)
    if both:
        b = Reduce(n, d, moe, got2, ss2, rs2)

        def put2(rows, total):
            moe_part[rows, :] = total.astype(bf16)

    a.send(0)
    gathers = [Gather(n, d, q, lambda i: q_all.at[i], qs, qr), Gather(n, d, o, lambda i: o_all.at[i], os, orr)]
    own = [pltpu.make_async_copy(q, q_all.at[d], loc.at[0]), pltpu.make_async_copy(o, o_all.at[d], loc.at[1])]
    for g in gathers:
        g.start()
    for c in own:
        c.start()
    a.recv(0, put)
    for j in range(1, steps):
        a.send(j)
        if both and j == 1:
            b.send(0)
        a.recv(j, put)
    z.start()
    if both:
        b.recv(0, put2)
        b.send(1)
    value = h1[...]
    dz = z.total()
    r = inv_rms(value)
    weighted = dz * gain[...]
    grad = r * weighted - value * (r * r * r) * jnp.mean(weighted * value, axis=-1, keepdims=True)
    grad = cot[pl.ds(t * z.share, z.share), :].astype(f32) + grad
    dh1[...] = grad
    low[...] = grad.astype(bf16)
    dh1r_all[t] = grad.astype(bf16)
    gain_part[...] = jnp.broadcast_to(jnp.sum(dz * value * r, axis=0, keepdims=True), gain_part.shape)
    x = Direct("tensor", nt, t, low, dh1r_all, xs, xr)
    x.start()
    for j in range(steps):
        for g in gathers:
            g.stage(j)
    if both:
        for j in range(1, steps):
            b.recv(j, put2)
            if j + 1 < steps:
                b.send(j + 1)
        b.finish()
    x.wait()
    for e in (a, z, x, *gathers):
        e.finish()
    for c in own:
        c.wait()


def leave(n, nt, dn2, moe, h1, cot, gain, q, o, cid):
    _, rows, cols = dn2.shape
    share = rows // nt
    sds, vm = jax.ShapeDtypeStruct, pltpu.VMEM
    both = moe is not None
    outs = [sds((share, cols), f32), sds((nt, share, cols), bf16), sds((8, cols), f32)] + [sds((n,) + q.shape, bf16)] * 2
    if both:
        outs.append(sds((rows, cols), bf16))
    got = [vm((2, n, rows // 2, cols), bf16)] * (2 if both else 1)
    sems = [DMA((2, n))] * (4 if both else 2) + [DMA((nt,))] * 4 + [DMA((2, n))] * 4 + [DMA((2,))]
    args = (dn2, h1, cot, gain, q, o) + ((moe,) if both else ())
    return kernel_call(
        functools.partial(leave_kernel, n, nt, both), "leave", cid, [VM] * 4 + [HB] * 2 + [VM] * both, outs, [VM] * 3 + [HB] * 2 + [VM] * both,
        got + [vm((rows, cols), bf16), vm((nt, share, cols), bf16), vm((share, cols), bf16)] + sems, args)


def fold_kernel(n, nt, p, out, got, ss, rs):
    d = lax.axis_index("dp")
    hello(dp_peers(n, d))

    def put(rows, total):
        out[rows, :] = total.astype(bf16)

    a = Reduce(n, d, p, got, ss, rs)
    for j in range(len(bit_list(n))):
        a.send(j)
        a.recv(j, put)
    a.finish()


def fold(n, nt, p, cid):
    _, rows, cols = p.shape
    return kernel_call(functools.partial(fold_kernel, n, nt), "fold", cid, [VM], jax.ShapeDtypeStruct((rows, cols), bf16), VM,
                       [pltpu.VMEM((2, n, rows // 2, cols), bf16), DMA((2, n)), DMA((2, n))], (p,))


def columns(row, lanes):
    return jnp.transpose(jnp.broadcast_to(row, (lanes, row.shape[1])))


def flat(x):
    return x.reshape(-1, x.shape[-1])


def back_kernel(n, nt, moe, h1, dh1r, dh1, hidden, gain, moe_gain_part, q, k, v, q_raw, k_raw, sums, q_gain, k_gain,
                cosine, sine, attended, lse, spot, spots, wq, wk, wv, wo, k_all, v_all, q_all, o_all, slices,
                out_all, grad_all, gains_out, q_grad, k_grad, v_grad, o_grad,
                wbuf, rbuf, do, do_all, terms, terms_all, rows, dq, dk, dlow, dall, sl_all, zgot, low, acc, part,
                cross, cross_all, gains, gpart, ggot, gsum, gall,
                loc, gs, gr, zs, zr, ns, nr, bs, br):
    d, t = lax.axis_index("dp"), lax.axis_index("tensor")
    heads = q.shape[1] // HD
    scale = HD ** (-0.5)
    steps = len(bit_list(n))
    cols = q.shape[1]
    greet(n, nt, d, t, True)
    loads = {}
    for i, (name, src, dst) in enumerate((("wo", wo, wbuf.at[3]), ("k", k_all, rbuf.at[0]), ("v", v_all, rbuf.at[1]),
                                          ("q", q_all, rbuf.at[2]), ("wv", wv, wbuf.at[2]), ("wq", wq, wbuf.at[0]),
                                          ("wk", wk, wbuf.at[1]), ("sl", slices.at[d], sl_all.at[d]), ("o", o_all, rbuf.at[0]))):
        loads[name] = pltpu.make_async_copy(src, dst, loc.at[i])
        if name != "o":
            loads[name].start()
    z1 = ZSum(nt, t, moe, zgot.at[0], zs.at[0], zr.at[0])
    z1.start()

    loads["wo"].wait()
    do[...] = contract(dh1r[...], wbuf[3], 1, 0).astype(bf16)
    do_all[d] = do[...]
    terms[0:8] = lse[...]
    terms[8:16] = jnp.zeros((8, terms.shape[1]), f32)
    deltas = []
    for h in range(heads):
        at = slice(h * HD, (h + 1) * HD)
        delta = jnp.sum(do[:, at].astype(f32) * attended[:, at], axis=1, keepdims=True)
        deltas.append(delta)
        terms[8 + h:9 + h] = across(delta, HD)[:1]
    terms_all[d] = terms[...]
    gathers = [Gather(n, d, do, lambda o: do_all.at[o], gs.at[0], gr.at[0]),
               Gather(n, d, terms, lambda o: terms_all.at[o], gs.at[1], gr.at[1])]
    for g in gathers:
        g.start()

    spots_row = [jnp.concatenate([spots[i, j:j + 1] for i in range(n)], axis=1) for j in (0, 1)]
    same = spot[:, 1:2] == spots_row[1]
    allowed = same & (spots_row[0] <= spot[:, 0:1])
    loads["k"].wait()
    loads["v"].wait()
    stage = 0
    for h in range(heads):
        at = slice(h * HD, (h + 1) * HD)
        keys, values = flat(rbuf[0, :, :, at]), flat(rbuf[1, :, :, at])
        score = scale * contract(q[:, at], keys, 1, 1)
        prob = jnp.where(allowed, jnp.exp(score - columns(lse[h:h + 1], HD)[:, :1]), 0.0)
        ds = (prob * (contract(do[:, at], values, 1, 1) - deltas[h])).astype(bf16)
        dq[:, at] = scale * contract(ds, keys, 1, 0)
        if h and stage < steps:
            for g in gathers:
                g.stage(stage)
            stage += 1
    for j in range(stage, steps):
        for g in gathers:
            g.stage(j)
    loads["o"].start()
    b = Direct("dp", n, d, slices, sl_all, bs.at[0], br.at[0], True)
    b.start()
    value = (h1[...] + z1.total()).astype(bf16)
    low[0] = value
    out_all[t] = value
    x1 = Direct("tensor", nt, t, low.at[0], out_all, ns.at[0], nr.at[0])
    x1.start()
    toks = terms.shape[1]
    for i in range(n):
        rows[:, i * toks:(i + 1) * toks] = terms_all[i]
    allowed = same & (spot[:, 0:1] <= spots_row[0])
    loads["q"].wait()
    for h in range(heads):
        at = slice(h * HD, (h + 1) * HD)
        queries, grads = flat(rbuf[2, :, :, at]), flat(do_all[:, :, at])
        score = scale * contract(k[:, at], queries, 1, 1)
        prob = jnp.where(allowed, jnp.exp(score - rows[h:h + 1]), 0.0)
        dlow[2, :, at] = contract(prob.astype(bf16), grads, 1, 0).astype(bf16)
        ds = (prob * (contract(v[:, at], grads, 1, 1) - rows[8 + h:9 + h])).astype(bf16)
        dk[:, at] = scale * contract(ds, queries, 1, 0)
    dall[2, d] = dlow[2]
    gv = Gather(n, d, dlow.at[2], lambda o: dall.at[2, o], gs.at[2], gr.at[2])
    gv.start()

    gains[...] = jnp.zeros(gains.shape, f32)
    gains[3:4] = moe_gain_part[0:1]
    inv = lax.rsqrt(sums[...] / D + EPSILON)
    invs = [columns(inv[i:i + 1], HD) for i in (0, 1)]
    cross_rows = []
    for i, (grad, raw, weight) in enumerate(((dq, q_raw, q_gain), (dk, k_raw, k_gain))):
        total = jnp.zeros((toks, 1), f32)
        for h in range(heads):
            at = slice(h * HD, (h + 1) * HD)
            y = grad[:, at]
            y = y * cosine[...] - pltpu.roll(y, HD // 2, 1) * sine[...]
            gains[1 + i:2 + i, pl.ds(pl.multiple_of(t * cols + h * HD, HD), HD)] = jnp.sum(
                y * raw[:, at] * invs[i], axis=0, keepdims=True)
            y = y * weight[:, at]
            total = total + jnp.sum(y * raw[:, at], axis=1, keepdims=True)
            grad[:, at] = y
        cross_rows.append(across(total, HD)[:8])
    row = lax.broadcasted_iota(jnp.int32, cross.shape, 0)
    value = jnp.where(row == 0, cross_rows[0], cross_rows[1])
    cross[...] = value
    cross_all[t] = value
    xc = Direct("tensor", nt, t, cross, cross_all, ns.at[1], nr.at[1])
    xc.start()
    loads["wv"].wait()
    acc[...] = contract(dlow[2], wbuf[2], 1, 1)
    gv.stage(0)
    xc.wait()
    total = cross_all[0]
    for i in range(1, nt):
        total = total + cross_all[i]
    gathers2 = []
    for i, (grad, raw) in enumerate(((dq, q_raw), (dk, k_raw))):
        factor = invs[i] * invs[i] * invs[i] * columns(total[i:i + 1], HD) / D
        for h in range(heads):
            at = slice(h * HD, (h + 1) * HD)
            dlow[i, :, at] = (invs[i] * grad[:, at] - raw[:, at] * factor).astype(bf16)
        dall[i, d] = dlow[i]
        g = Gather(n, d, dlow.at[i], lambda o, i=i: dall.at[i, o], gs.at[3 + i], gr.at[3 + i])
        g.start()
        gathers2.append(g)
    loads["wq"].wait()
    loads["wk"].wait()
    part[...] = (acc[...] + contract(dlow[0], wbuf[0], 1, 1) + contract(dlow[1], wbuf[1], 1, 1)).astype(bf16)
    z2 = ZSum(nt, t, part, zgot.at[1], zs.at[1], zr.at[1])
    z2.start()
    gathers2.append(gv)
    for j in range(steps):
        for g in gathers2:
            if j or g is not gv:
                g.stage(j)
    b.wait()
    loads["sl"].wait()
    loads["o"].wait()
    normed_all, dh1r_all = flat(sl_all[:, :toks]), flat(sl_all[:, toks:])
    o_grad[...] = contract(dh1r_all, flat(rbuf[0]), 0, 0)
    dz = z2.total()
    value = hidden[pl.ds(t * z2.share, z2.share), :].astype(f32)
    r = inv_rms(value)
    weighted = dz * gain[...]
    grad = r * weighted - value * (r * r * r) * jnp.mean(weighted * value, axis=-1, keepdims=True)
    grad = (dh1[...] + grad).astype(bf16)
    low[1] = grad
    grad_all[t] = grad
    x2 = Direct("tensor", nt, t, low.at[1], grad_all, ns.at[2], nr.at[2])
    x2.start()
    gains[0:1] = jnp.sum(dz * value * r, axis=0, keepdims=True)
    width = gpart.shape[2]
    for i in range(n):
        gpart[i] = gains[:, i * width:(i + 1) * width]
    p = Direct("dp", n, d, gpart, ggot, bs.at[1], br.at[1], True)
    p.start()
    for i, out in enumerate((q_grad, k_grad, v_grad)):
        out[...] = contract(normed_all, flat(dall[i]), 0, 0)
    p.wait()
    total = gpart[d]
    for m in range(1, n):
        total = total + ggot[flip(d, m)]
    gsum[...] = total
    gall[t] = total
    xg = Direct("tensor", nt, t, gsum, gall, ns.at[3], nr.at[3])
    xg.start()
    x1.wait()
    xg.wait()
    total = gall[0]
    for i in range(1, nt):
        total = total + gall[i]
    gains_out[...] = total
    x2.wait()
    for e in (z1, z2, x1, xc, x2, xg, b, p, *gathers, *gathers2):
        e.finish()


def back(n, nt, in_vmem, in_hbm, cid):
    moe, q, slices = in_vmem[0], in_vmem[7], in_hbm[-1]
    toks, cols = q.shape
    dim = moe.shape[1]
    share, width = toks // nt, dim // n
    sds, vm = jax.ShapeDtypeStruct, pltpu.VMEM
    return kernel_call(
        functools.partial(back_kernel, n, nt), "back", cid, [VM] * len(in_vmem) + [HB] * len(in_hbm),
        [sds((nt, share, dim), bf16)] * 2 + [sds((8, width), f32)] + [sds((width, cols), f32)] * 4, [VM] * 7,
        [vm((4, dim, cols), bf16), vm((3, n, toks, cols), bf16), vm((toks, cols), bf16), vm((n, toks, cols), bf16),
         vm((16, toks), f32), vm((n, 16, toks), f32), vm((16, n * toks), f32), vm((toks, cols), f32), vm((toks, cols), f32),
         vm((3, toks, cols), bf16), vm((3, n, toks, cols), bf16), vm(slices.shape, bf16), vm((2, nt, share, dim), bf16),
         vm((2, share, dim), bf16), vm((toks, dim), f32), vm((toks, dim), bf16), vm((8, toks), f32), vm((nt, 8, toks), f32),
         vm((8, dim), f32), vm((n, 8, width), f32), vm((n, 8, width), f32), vm((8, width), f32), vm((nt, 8, width), f32),
         DMA((9,)), DMA((5, 2, n)), DMA((5, 2, n)), DMA((2, nt)), DMA((2, nt)), DMA((4, nt)), DMA((4, nt)), DMA((2, n)), DMA((2, n))],
        (*in_vmem, *in_hbm))


def weight_grad_kernel(order, a_ref, b_ref, out_ref):
    per = b_ref.shape[2] // 128
    for i in range(b_ref.shape[0]):
        res = contract(a_ref[...], b_ref[i], 0, 0)
        for f in range(per):
            out_ref[pl.ds(order[i * per + f], res.shape[0], stride=len(order)), :] = res[:, f * 128:(f + 1) * 128]


def weight_grad(a, b, order):
    toks, rows = a.shape
    block = 256
    return pl.pallas_call(
        functools.partial(weight_grad_kernel, order),
        grid=(rows // block,),
        in_specs=[pl.BlockSpec((toks, block), lambda i: (0, i)), pl.BlockSpec(b.shape, lambda i: (0, 0, 0))],
        out_specs=pl.BlockSpec((block * len(order), 128), lambda i: (i, 0)),
        out_shape=jax.ShapeDtypeStruct((rows * len(order), 128), f32),
        name="weight_grad",
    )(a, b)


D = 2048
HD = 128
TOPK = 8
EPSILON = 1e-05
ROPE_BASE = 10000.0
NEG_FILL = -1e30


def norm_back(values, gain, grad_out):
    inv_rms = lax.rsqrt(jnp.mean(values * values, axis=-1, keepdims=True) + EPSILON)
    weighted = grad_out * gain
    grad_in = inv_rms * weighted - values * inv_rms**3 * jnp.mean(weighted * values, axis=-1, keepdims=True)
    return grad_in, jnp.sum(grad_out * values * inv_rms, axis=0)


def locate(anchor, lengths):
    ends = jnp.cumsum(lengths)
    starts = ends - lengths
    docs = jnp.sum((anchor[:, None] >= ends[None, :]).astype(jnp.int32), axis=1)
    which = docs[:, None] == jnp.arange(lengths.shape[0], dtype=jnp.int32)[None, :]
    begins = jnp.sum(jnp.where(which, starts[None, :], 0), axis=1)
    return docs, (anchor - begins).astype(jnp.int32)


def rope_tables(positions):
    half_dim = HD // 2
    freqs = ROPE_BASE ** (-2.0 * jnp.arange(half_dim, dtype=f32) / HD)
    angles = positions.astype(f32)[:, None] * freqs[None, :]
    cosine, sine = jnp.cos(angles), jnp.sin(angles)
    return jnp.concatenate([cosine, cosine], axis=1)[:, None, :], jnp.concatenate([-sine, sine], axis=1)[:, None, :]


def turn(x, cosine, sine):
    return x * cosine + jnp.roll(x, HD // 2, axis=-1) * sine


def pair_allowed(query_anchor, query_docs, key_anchor, key_docs):
    return ((query_docs[:, None] == key_docs[None, :]) & (key_anchor[None, :] <= query_anchor[:, None]))[None]


def contract(left, right, l, r):
    return lax.dot_general(left, right, (((l,), (r,)), ((), ())), preferred_element_type=f32)


def routing(experts, gates, num_exp, capacity):
    toks = experts.shape[0]
    chosen = experts[:, :, None] == jnp.arange(num_exp, dtype=jnp.int32)[None, None, :]
    mask = jnp.any(chosen, axis=1)
    gate = jnp.sum(jnp.where(chosen, gates[:, :, None], 0.0), axis=1)
    index = jnp.arange(toks, dtype=jnp.int32)
    before = (index[:, None] > index[None, :]).astype(bf16)
    slot = contract(before, mask.astype(bf16), 1, 0)
    return jnp.where(mask & (slot < capacity), gate, 0.0)


def small(rows):
    rows = jnp.stack(rows)
    return jnp.pad(rows, ((0, -rows.shape[0] % 8), (0, 0)))


def shards(hidden_in, attn_gain, query_weight, key_weight, value_weight, output_weight, query_gain, key_gain,
           moe_gain, expert_gate_up, expert_down, experts, gates, anchor, lengths, cotangent):
    n, nt = lax.axis_size("dp"), lax.axis_size("tensor")
    d, t = lax.axis_index("dp"), lax.axis_index("tensor")
    toks = hidden_in.shape[0]
    share = toks // nt
    cols = query_weight.shape[1]
    heads = cols // HD
    scale = HD ** (-0.5)
    exp_local = expert_down.shape[1]
    num_exp = exp_local * n
    capacity = 9 * toks * TOPK // (8 * num_exp)
    hidden = hidden_in.astype(f32)

    def mine(a):
        return lax.dynamic_slice_in_dim(a, t * share, share, 0)

    coef = routing(experts, gates, num_exp, capacity).T
    place = jnp.broadcast_to(anchor[None, :], (16, toks))
    wq, wk, wv, anchor_all = gather_dp(n, (query_weight, key_weight, value_weight, place), 1)
    wq, wk, wv = (w.reshape(D, cols) for w in (wq, wk, wv))
    anchor_all = anchor_all[:, 0].reshape(n * toks)

    docs, positions = locate(anchor, lengths)
    docs_all, _ = locate(anchor_all, lengths)
    cosine, sine = rope_tables(positions)
    allowed = pair_allowed(anchor, docs, anchor_all, docs_all)

    inv = lax.rsqrt(jnp.mean(hidden * hidden, axis=-1, keepdims=True) + EPSILON)
    normed = (hidden * inv * attn_gain).astype(bf16)
    q_raw, k_raw, v_raw = (contract(normed, w, 1, 0) for w in (wq, wk, wv))
    v = v_raw.astype(bf16)
    q, k, k_all, v_all, wo, sq = mix(
        n, nt, q_raw, k_raw, v, cosine[:, 0], sine[:, 0], query_gain[None, :], key_gain[None, :], output_weight, 2)
    wo = wo.reshape(D, cols)
    q_flat, k_flat, v_flat, k_flat_all, v_flat_all = q, k, v, k_all, v_all
    q, k, v = (a.reshape(toks, heads, HD) for a in (q, k, v))
    k_all, v_all = (a.reshape(n * toks, heads, HD) for a in (k_all, v_all))

    scores = scale * jnp.einsum("qhd,khd->hqk", q, k_all, preferred_element_type=f32)
    top = jnp.max(jnp.where(allowed, scores, NEG_FILL), axis=2)
    probs = jnp.where(allowed, jnp.exp(scores - top[:, :, None]), 0.0)
    total = jnp.sum(probs, axis=2)
    lse = top + jnp.log(total)
    attended = jnp.einsum("hqk,khd->qhd", probs.astype(bf16), v_all, preferred_element_type=f32)
    attended = attended / total.T[:, :, None]
    o = attended.reshape(toks, cols).astype(bf16)
    n2_all, h1, dy_all, coef_all = enter(
        n, nt, contract(o, wo, 1, 1).astype(bf16), hidden_in, moe_gain[None, :], cotangent, coef, 4)
    n2_all, dy_all = n2_all.reshape(n * toks, D), dy_all.reshape(n * toks, D)
    coef_all = lax.dynamic_slice_in_dim(coef_all, d * exp_local, exp_local, 1)
    coef_all = coef_all.transpose(1, 0, 2).reshape(exp_local, n * toks, 1)

    gu = jnp.einsum("td,dezf->eztf", n2_all, expert_gate_up, preferred_element_type=f32)
    g, u = gu[:, 0], gu[:, 1]
    sig = jax.nn.sigmoid(g)
    act = (coef_all * (g * sig * u)).astype(bf16)
    dact = coef_all * jnp.einsum("td,def->etf", dy_all, expert_down, preferred_element_type=f32)
    dgu = jnp.stack([dact * u * sig * (1.0 + g * (1.0 - sig)), dact * (g * sig)], axis=1).astype(bf16)
    act, dgu = lax.optimization_barrier((act, dgu))
    dn2 = jnp.einsum("eztf,dezf->td", dgu, expert_gate_up, preferred_element_type=f32).astype(bf16)
    moe = jnp.einsum("etf,def->td", act, expert_down, preferred_element_type=f32).astype(bf16)
    half = expert_down.shape[2] // 128
    down_grad = weight_grad(dy_all, act, [f * exp_local + e for e in range(exp_local) for f in range(half)])
    down_grad = down_grad.reshape(D, half, exp_local, 128).transpose(0, 2, 1, 3).reshape(expert_down.shape)
    gate_up_grad = weight_grad(n2_all, dgu.reshape(2 * exp_local, n * toks, -1),
                               [(e * half + f) * 2 + z for e in range(exp_local) for z in (0, 1) for f in range(half)])
    gate_up_grad = gate_up_grad.reshape(D, exp_local, half, 2, 128).transpose(0, 1, 3, 2, 4).reshape(expert_gate_up.shape)

    dn2, moe = dn2.reshape(n, toks, D), moe.reshape(n, toks, D)
    together = 16 * n * toks * D <= 48 * 2**20
    dh1, dh1r, moe_gain_part, q_all, o_all, *rest = leave(
        n, nt, dn2, moe if together else None, h1, cotangent, moe_gain[None, :], q_flat, o, 6)
    moe = rest[0] if together else fold(n, nt, moe, 7)
    dh1r = dh1r.reshape(toks, D)

    slices = jnp.concatenate([normed, dh1r], axis=0).reshape(2 * toks, n, D // n).transpose(1, 0, 2)
    spot = jnp.stack([anchor, docs], axis=1)
    spots = jnp.stack([anchor_all, docs_all], axis=0).reshape(2, n, toks).transpose(1, 0, 2)
    output, input_grad, gains, query_grad, key_grad, value_grad, output_grad = back(
        n, nt,
        (moe, h1, dh1r, dh1, hidden_in, attn_gain[None, :], moe_gain_part, q_flat, k_flat, v_flat, q_raw, k_raw, sq,
         query_gain[None, :], key_gain[None, :], cosine[:, 0], sine[:, 0], attended.reshape(toks, cols), small(list(lse)), spot, spots),
        (wq, wk, wv, wo, k_flat_all, v_flat_all, q_all, o_all, slices), 9)
    output = output.reshape(toks, D)
    input_grad = input_grad.reshape(toks, D).astype(f32)
    return (output, input_grad, query_grad, key_grad, value_grad, output_grad, gate_up_grad, down_grad,
            gains[0], gains[1], gains[2], gains[3])


def solution(mesh):
    in_specs = (
        P("dp", None),
        P(),
        P("dp", "tensor"),
        P("dp", "tensor"),
        P("dp", "tensor"),
        P("dp", "tensor"),
        P("tensor"),
        P("tensor"),
        P(),
        P(None, "dp", None, "tensor"),
        P(None, "dp", "tensor"),
        P("dp", None),
        P("dp", None),
        P("dp"),
        P(),
        P("dp", None),
    )
    out_specs = (
        P("dp", None),
        P("dp", None),
        P("dp", "tensor"),
        P("dp", "tensor"),
        P("dp", "tensor"),
        P("dp", "tensor"),
        P(None, "dp", None, "tensor"),
        P(None, "dp", "tensor"),
        P("dp"),
        P("dp"),
        P("dp"),
        P("dp"),
    )
    return jax.shard_map(shards, mesh=mesh, in_specs=in_specs, out_specs=out_specs, check_vma=False)
```
